256 devices in a mesh: owner: 16 (over z_lo, y), rows: 16 (over z_hi, x, core).
Axes of the slice: x: 4, y: 4, z: 8 (z_hi: 2, z_lo: 4; z = z_hi * 4 + z_lo), core: 2. Of those that a mesh axis runs over, the one named last changes fastest.
Arguments:
- master_down: float32 [16, 6400, 4096], P('owner', None, 'rows'), may hold values from -0.109375 to 0.109375
- router_weight: float32 [4096, 16], P('rows', 'owner'), may hold values from -0.09375 to 0.09375
- router_gain: float32 [4096], P('rows'), may hold values from 0.25 to 1.75
Outputs:
- final_down: bfloat16 [16, 6400, 4096], P('owner', 'rows')
- scale_down: float32 [16, 6400], P('owner', 'rows')
- serve_router: bfloat16 [4096, 16], replicated
The draws below stay inside these ranges and needn't reach their ends.
All inputs are finite; a program needn't handle non-finite values. Where the reference program divides by a largest or mean magnitude, that divisor is 1e-20 or more.
Results may differ from the reference program's by a relative error of at most 0.001.
Values may be sent and summed in bfloat16 or wider, within the bound.
A program may use at most 64 MiB of HBM per device.

```python
import jax
import jax.numpy as jnp

EXPERTS = 16
D_MODEL = 4096
D_EXPERT = 6400


def with_spikes(entries, rng, source, target, blocks, factor):
    owner, partner = [(jnp.arange(entries.shape[position]) // (entries.shape[position] // blocks)).reshape([-1 if axis == position else 1 for axis in range(entries.ndim)]) for position in (source, target)]
    chosen = jax.random.permutation(rng, blocks)[partner]
    strong = (owner == chosen) | (owner == (partner + blocks // 2) % blocks)
    return jnp.where(strong, factor * entries, entries)


def level_of(key, dims, cuts, low, largest):
    def one(axis_at, shards_of):
        heights = jax.random.uniform(jax.random.fold_in(jax.random.fold_in(key, 6), axis_at), (shards_of,), jnp.float32, low / len(cuts), largest / len(cuts))
        return jnp.repeat(jnp.exp(heights), dims[axis_at] // shards_of).reshape((-1,) + (1,) * (len(dims) - axis_at - 1))

    level = one(*cuts[0])
    for cut in cuts[1:]:
        level = level * one(*cut)
    return level


def gaussian(own_key, extent, deviation, bound, shards=(), dtype=jnp.bfloat16):
    drawn = deviation * jax.random.normal(own_key, extent, jnp.float32)
    if shards:
        drawn = drawn * level_of(own_key, extent, shards, -0.22, 0.18)
    return jnp.clip(drawn, -bound, bound).astype(dtype)


def heavy_noise(rng, dims, spread, bound, split, heavy, held_as=jnp.bfloat16):
    entries = spread * jax.random.normal(rng, dims, jnp.float32)
    if split:
        entries = entries * level_of(rng, dims, split, -0.22, 0.18)
    return jnp.clip(with_spikes(entries, jax.random.fold_in(rng, 3), *heavy), -bound, bound).astype(held_as)


def setup_inputs(seed: int = 0) -> dict:
    key_list = jax.random.split(jax.random.key(seed), 4)
    return {
        "master_down": heavy_noise(key_list[0], (EXPERTS, D_EXPERT, D_MODEL), D_EXPERT ** -0.5, 0.109375, ((0, 16), (2, 16)), (2, 1, 16, 2.0), jnp.float32),
        "router_weight": gaussian(key_list[1], (D_MODEL, EXPERTS), D_MODEL ** -0.5, 0.09375, ((0, 16), (1, 16)), jnp.float32),
        "router_gain": jnp.clip(1.0 + 0.15 * jax.random.normal(key_list[2], (D_MODEL,), jnp.float32), 0.25, 1.75),
    }


def reference(master_down, router_weight, router_gain):
    scale_down = jnp.sum(jnp.abs(master_down), axis=2) / D_MODEL
    final_down = (master_down / jnp.expand_dims(scale_down, 2)).astype(jnp.bfloat16)
    serve_router = (router_weight * router_gain[:, None]).astype(jnp.bfloat16)
    return final_down, scale_down, serve_router
```

```python
import functools

import jax
import jax.numpy as jnp
from jax import lax
from jax.experimental import pallas as pl
from jax.experimental.pallas import tpu as pltpu
from jax.sharding import PartitionSpec as P

MESH = pl.DeviceIdType.MESH
N = 16
ROWS = 400
COLS = 256
WIDTH = 4096
TILES = ROWS // 8

FAR = [(1, dx, dc) for dx in (0, 2, 1, 3) for dc in (0, 1)]
NEAR = [(0, dx, dc) for dx in (2, 1, 3) for dc in (0, 1)] + [(0, 0, 1)]
PEERS = FAR + NEAR
BACK = [PEERS.index((h, (4 - dx) % 4, dc)) for h, dx, dc in PEERS]
OWNERS = [(dz, dy) for dz in range(4) for dy in range(4)][1:]


def peer_row(me, step):
    half, dx, dc = step
    x = lax.rem(lax.rem(me // 2, 4) + dx, 4)
    return lax.rem(me // 8 + half, 2) * 8 + x * 2 + lax.rem(lax.rem(me, 2) + dc, 2)


def peer_owner(me, step):
    return lax.rem(me // 4 + step[0], 4) * 4 + lax.rem(lax.rem(me, 4) + step[1], 4)


def sums_of(block):
    part = jnp.sum(jnp.abs(block), axis=1, keepdims=True).reshape(TILES, 8, 1)
    shape = (TILES, 8, 128)
    place = lax.broadcasted_iota(jnp.int32, shape, 0) == lax.broadcasted_iota(jnp.int32, shape, 2)
    return jnp.sum(jnp.where(place, part, 0.0), axis=0)


def scaled(master, first, inverse, k):
    block = master[pl.ds(pl.multiple_of(first + 16 * k, 16), 16), :]
    by = jnp.concatenate(
        [jnp.broadcast_to(inverse[:, c : c + 1], (8, COLS)) for c in (2 * k, 2 * k + 1)], axis=0
    )
    return (block * by).astype(jnp.bfloat16)


def kernel(
    master_hbm, weight, gain, final, scale, router,
    master, narrow, sums, parts, totals, row, column,
    in_sem, part_s, part_r, total_s, total_r, tile_s, tile_r, row_s, row_r, pair_s, pair_r, half_s, half_r,
):
    me, owner = lax.axis_index("rows"), lax.axis_index("owner")
    rows_of = [peer_row(me, step) for step in PEERS]
    owners_of = [peer_owner(owner, step) for step in OWNERS]

    def send(src, dst, send_sem, recv_sem, to_owner, to_row):
        copy = pltpu.make_async_remote_copy(
            src_ref=src, dst_ref=dst, send_sem=send_sem, recv_sem=recv_sem,
            device_id=(to_owner, to_row), device_id_type=MESH,
        )
        copy.start()
        return copy

    def tile_at(device):
        return pl.ds(pl.multiple_of(device * ROWS, ROWS), ROWS)

    def columns_at(device):
        return pl.ds(pl.multiple_of(device * COLS, COLS), COLS)

    loads = []
    for d in range(N):
        load = pltpu.make_async_copy(
            master_hbm.at[0, pl.ds(d * ROWS, ROWS), :], master.at[pl.ds(d * ROWS, ROWS), :], in_sem.at[d]
        )
        load.start()
        loads.append(load)

    barrier = pltpu.get_barrier_semaphore()
    for r in rows_of:
        pl.semaphore_signal(barrier, inc=1, device_id=(owner, r), device_id_type=MESH)
    for o in owners_of:
        pl.semaphore_signal(barrier, inc=1, device_id=(o, me), device_id_type=MESH)

    row[...] = (weight[...] * gain[...])[None]
    for d in range(N):
        loads[d].wait()
        sums[d] = sums_of(master[pl.ds(d * ROWS, ROWS), :])
    pl.semaphore_wait(barrier, len(rows_of) + len(owners_of))

    waits = []
    part_copies = [
        send(sums.at[r], parts.at[me], part_s.at[i], part_r.at[i], owner, r) for i, r in enumerate(rows_of)
    ]
    row_copies = [
        send(row.at[0], column.at[owner], row_s.at[i], row_r.at[i], o, me) for i, o in enumerate(owners_of)
    ]
    parts[me] = sums[me]
    column[owner] = row[0]
    for copy in part_copies:
        copy.wait_recv()
    total = parts[0]
    for d in range(1, N):
        total = total + parts[d]
    totals[me] = total / WIDTH
    total_copies = [
        send(totals.at[me], totals.at[me], total_s.at[i], total_r.at[i], owner, r) for i, r in enumerate(rows_of)
    ]

    for copy in row_copies:
        copy.wait_recv()
    router[:, columns_at(me)] = jnp.concatenate([column[o] for o in range(N)], axis=0).astype(jnp.bfloat16)
    across = rows_of[0]

    mean = totals[me]
    shape = (128, 512)
    spread = (lax.broadcasted_iota(jnp.int32, shape, 1) // 8 == lax.broadcasted_iota(jnp.int32, shape, 0)).astype(jnp.float32)
    wide = jnp.dot(mean, spread, precision=lax.Precision.HIGHEST, preferred_element_type=jnp.float32)
    shape = (8, 512)
    keep = lax.rem(lax.broadcasted_iota(jnp.int32, shape, 1), 8) == lax.broadcasted_iota(jnp.int32, shape, 0)
    scale[...] = jnp.sum(jnp.where(keep, wide, 0.0), axis=0, keepdims=True)[:, :ROWS]

    pair = send(
        router.at[:, columns_at(me)], router.at[:, columns_at(me)], pair_s.at[0], pair_r.at[0], owner, across
    )

    def scale_tile(device, store):
        inverse = 1.0 / jnp.where(lax.broadcasted_iota(jnp.int32, (8, 128), 1) < TILES, totals[device], 1.0)
        for k in range(ROWS // 16):
            store(k, scaled(master, device * ROWS, inverse, k))

    def to_narrow(device):
        def store(k, value):
            narrow[pl.ds(pl.multiple_of(device * ROWS + 16 * k, 16), 16), :] = value

        return store

    tile_copies, half_copies = [], []
    for i, r in enumerate(rows_of):
        total_copies[BACK[i]].wait_recv()
        scale_tile(r, to_narrow(r))
        tile_copies.append(
            send(narrow.at[tile_at(r), :], final.at[:, columns_at(me)], tile_s.at[i], tile_r.at[i], owner, r)
        )
        if i == 1:
            pair.wait_recv()
            for j in range(len(NEAR)):
                for k, block in enumerate((me, across)):
                    half_copies.append(
                        send(
                            router.at[:, columns_at(block)], router.at[:, columns_at(block)],
                            half_s.at[j, k], half_r.at[j, k], owner, rows_of[len(FAR) + j],
                        )
                    )

    def to_final(k, value):
        final[16 * k : 16 * k + 16, columns_at(me)] = value

    scale_tile(me, to_final)
    for copy in part_copies + row_copies + total_copies + [pair]:
        copy.wait_send()
    for copy in half_copies + tile_copies:
        copy.wait()


def per_device(master_down, router_weight, router_gain):
    vmem = pl.BlockSpec(memory_space=pltpu.VMEM)
    dma = pltpu.SemaphoreType.DMA
    final, scale, router = pl.pallas_call(
        kernel,
        out_shape=(
            jax.ShapeDtypeStruct((ROWS, WIDTH), jnp.bfloat16),
            jax.ShapeDtypeStruct((1, ROWS), jnp.float32),
            jax.ShapeDtypeStruct((N, WIDTH), jnp.bfloat16),
        ),
        in_specs=[pl.BlockSpec(memory_space=pltpu.HBM), vmem, vmem],
        out_specs=(vmem, vmem, vmem),
        scratch_shapes=[
            pltpu.VMEM((N * ROWS, COLS), jnp.float32),
            pltpu.VMEM((N * ROWS, COLS), jnp.bfloat16),
            pltpu.VMEM((N, 8, 128), jnp.float32),
            pltpu.VMEM((N, 8, 128), jnp.float32),
            pltpu.VMEM((N, 8, 128), jnp.float32),
            pltpu.VMEM((1, 1, COLS), jnp.float32),
            pltpu.VMEM((N, 1, COLS), jnp.float32),
            dma((N,)),
            dma((len(PEERS),)), dma((len(PEERS),)),
            dma((len(PEERS),)), dma((len(PEERS),)),
            dma((len(PEERS),)), dma((len(PEERS),)),
            dma((len(OWNERS),)), dma((len(OWNERS),)),
            dma((1,)), dma((1,)),
            dma((len(NEAR), 2)), dma((len(NEAR), 2)),
        ],
        compiler_params=pltpu.CompilerParams(
            collective_id=0, has_side_effects=True, vmem_limit_bytes=48 << 20
        ),
    )(master_down, router_weight.reshape(1, COLS), router_gain.reshape(1, COLS))
    return final[None], scale, router.T


def solution(mesh):
    return jax.shard_map(
        per_device,
        mesh=mesh,
        in_specs=(P("owner", None, "rows"), P("rows", "owner"), P("rows")),
        out_specs=(P("owner", "rows", None), P("owner", "rows"), P()),
        check_vma=False,
    )
```

```python
import jax
import jax.numpy as jnp
from jax import lax
from jax.experimental import pallas as pl
from jax.experimental.pallas import tpu as pltpu
from jax.sharding import PartitionSpec as P

MESH = pl.DeviceIdType.MESH
N = 16
HALF = 8
ROWS = 400
COLS = 256
WIDTH = 4096
TILES = ROWS // 8
RAW = 0

FAR = [(1, dx, dc) for dx in (0, 2, 1, 3) for dc in (0, 1)]
NEAR = [(0, dx, dc) for dx in (2, 1, 3) for dc in (0, 1)] + [(0, 0, 1)]
PEERS = FAR + NEAR
BACK = [NEAR.index((h, (4 - dx) % 4, dc)) for h, dx, dc in NEAR]
OWNERS = [(dz, dy) for dz in range(4) for dy in range(4)][1:]


def peer_row(me, step):
    half, dx, dc = step
    x = lax.rem(lax.rem(me // 2, 4) + dx, 4)
    return lax.rem(me // 8 + half, 2) * 8 + x * 2 + lax.rem(lax.rem(me, 2) + dc, 2)


def peer_owner(me, step):
    return lax.rem(me // 4 + step[0], 4) * 4 + lax.rem(lax.rem(me, 4) + step[1], 4)


def sums_of(block, at):
    part = jnp.sum(jnp.abs(block), axis=1, keepdims=True).reshape(TILES, 8, 1)
    shape = (TILES, 8, 128)
    place = lax.broadcasted_iota(jnp.int32, shape, 0) + at == lax.broadcasted_iota(jnp.int32, shape, 2)
    return jnp.sum(jnp.where(place, part, 0.0), axis=0)


def scaled(block, inverse, k):
    by = jnp.concatenate(
        [jnp.broadcast_to(inverse[:, c : c + 1], (8, COLS)) for c in (2 * k, 2 * k + 1)], axis=0
    )
    return (block * by).astype(jnp.bfloat16)


def kernel(
    master_hbm, product, final, scale, router,
    master, narrow, sums, parts, totals, raw, row, column,
    in_sem, part_s, part_r, total_s, total_r, tile_s, tile_r, row_s, row_r, pair_s, pair_r, half_s, half_r, raw_s, raw_r,
):
    me, owner = lax.axis_index("rows"), lax.axis_index("owner")
    rows_of = [peer_row(me, step) for step in PEERS]
    owners_of = [peer_owner(owner, step) for step in OWNERS]
    across = rows_of[0]
    pair_of = lambda device: lax.rem(device, HALF)

    def send(src, dst, send_sem, recv_sem, to_owner, to_row):
        copy = pltpu.make_async_remote_copy(
            src_ref=src, dst_ref=dst, send_sem=send_sem, recv_sem=recv_sem,
            device_id=(to_owner, to_row), device_id_type=MESH,
        )
        copy.start()
        return copy

    def columns_at(device):
        return pl.ds(pl.multiple_of(device * COLS, COLS), COLS)

    loads = []
    for d in range(N):
        load = pltpu.make_async_copy(
            master_hbm.at[0, pl.ds(d * ROWS, ROWS), :], master.at[pl.ds(d * ROWS, ROWS), :], in_sem.at[d]
        )
        load.start()
        loads.append(load)

    barrier = pltpu.get_barrier_semaphore()
    for r in rows_of:
        pl.semaphore_signal(barrier, inc=1, device_id=(owner, r), device_id_type=MESH)
    for o in owners_of:
        pl.semaphore_signal(barrier, inc=1, device_id=(o, me), device_id_type=MESH)

    row[...] = product[...][None]
    held = {}
    for d in range(N):
        loads[d].wait()
        held[d] = sums_of(master[pl.ds(d * ROWS, ROWS), :], 0 if d < HALF else TILES)
        if d >= HALF:
            sums[d - HALF] = held[d - HALF] + held[d]
    pl.semaphore_wait(barrier, len(rows_of) + len(owners_of))

    part_copies = [
        send(sums.at[pair_of(r)], parts.at[me], part_s.at[i], part_r.at[i], owner, r) for i, r in enumerate(rows_of)
    ]
    row_copies = [
        send(row.at[0], column.at[owner], row_s.at[i], row_r.at[i], o, me) for i, o in enumerate(owners_of)
    ]
    raw_copies = []
    if RAW:
        raw_copies.append(
            send(
                master.at[pl.ds(pl.multiple_of(across * ROWS, ROWS), RAW), :], raw, raw_s.at[0], raw_r.at[0], owner, across
            )
        )
    parts[me] = sums[pair_of(me)]
    column[owner] = row[0]
    for copy in part_copies:
        copy.wait_recv()
    total = parts[0]
    for d in range(1, N):
        total = total + parts[d]
    totals[pair_of(me)] = total / WIDTH
    total_copies = [
        send(
            totals.at[pair_of(me)], totals.at[pair_of(me)], total_s.at[i], total_r.at[i], owner, rows_of[len(FAR) + i]
        )
        for i in range(len(NEAR))
    ]

    def mean_of(device):
        both = totals[pair_of(device)]
        return jnp.where(device // HALF == 1, pltpu.roll(both, 128 - TILES, 1), both)

    def inverse_of(device):
        return 1.0 / jnp.where(lax.broadcasted_iota(jnp.int32, (8, 128), 1) < TILES, mean_of(device), 1.0)

    tile_copies = []

    def send_tile(i):
        device, first = rows_of[i], RAW if i == 0 else 0
        inverse = inverse_of(device)
        for k in range(first // 16, ROWS // 16):
            at = pl.ds(pl.multiple_of(device * ROWS + 16 * k, 16), 16)
            narrow[at, :] = scaled(master[at, :], inverse, k)
        tile_copies.append(
            send(
                narrow.at[pl.ds(pl.multiple_of(device * ROWS + first, 16), ROWS - first), :],
                final.at[pl.ds(first, ROWS - first), columns_at(me)],
                tile_s.at[i], tile_r.at[i], owner, device,
            )
        )

    arrived = set()

    def have_total(i):
        near = NEAR.index((0,) + PEERS[i][1:]) if PEERS[i][1:] != (0, 0) else None
        if near is not None and near not in arrived:
            total_copies[BACK[near]].wait_recv()
            arrived.add(near)

    for i in range(len(PEERS)):
        have_total(i)
        send_tile(i)
        if i == 1:
            for copy in row_copies:
                copy.wait_recv()
            router[:, columns_at(me)] = jnp.concatenate([column[o] for o in range(N)], axis=0).astype(jnp.bfloat16)
        if i == 2:
            pair = send(
                router.at[:, columns_at(me)], router.at[:, columns_at(me)], pair_s.at[0], pair_r.at[0], owner, across
            )

    own = inverse_of(me)
    for k in range(ROWS // 16):
        block = master[pl.ds(pl.multiple_of(me * ROWS + 16 * k, 16), 16), :]
        final[16 * k : 16 * k + 16, columns_at(me)] = scaled(block, own, k)

    shape = (128, 512)
    spread = (lax.broadcasted_iota(jnp.int32, shape, 1) // 8 == lax.broadcasted_iota(jnp.int32, shape, 0)).astype(jnp.float32)
    wide = jnp.dot(mean_of(me), spread, precision=lax.Precision.HIGHEST, preferred_element_type=jnp.float32)
    shape = (8, 512)
    keep = lax.rem(lax.broadcasted_iota(jnp.int32, shape, 1), 8) == lax.broadcasted_iota(jnp.int32, shape, 0)
    scale[...] = jnp.sum(jnp.where(keep, wide, 0.0), axis=0, keepdims=True)[:, :ROWS]

    for copy in raw_copies:
        copy.wait_recv()
        for k in range(RAW // 16):
            final[16 * k : 16 * k + 16, columns_at(across)] = scaled(raw[16 * k : 16 * k + 16, :], own, k)

    pair.wait_recv()
    half_copies = []
    for j in range(len(NEAR)):
        for k, block in enumerate((me, across)):
            half_copies.append(
                send(
                    router.at[:, columns_at(block)], router.at[:, columns_at(block)],
                    half_s.at[j, k], half_r.at[j, k], owner, rows_of[len(FAR) + j],
                )
            )
    for copy in part_copies + row_copies + total_copies + raw_copies + [pair]:
        copy.wait_send()
    for copy in half_copies + tile_copies:
        copy.wait()


def put(a, b, c, out_a, out_b, out_c, sem):
    copies = [pltpu.make_async_copy(src, dst, sem.at[i]) for i, (src, dst) in enumerate(((a, out_a), (b, out_b), (c, out_c)))]
    for copy in copies:
        copy.start()
    for copy in copies:
        copy.wait()


def per_device(master_down, router_weight, router_gain):
    vmem, hbm = pl.BlockSpec(memory_space=pltpu.VMEM), pl.BlockSpec(memory_space=pl.ANY)
    dma = pltpu.SemaphoreType.DMA
    peers, near, owners = len(PEERS), len(NEAR), len(OWNERS)
    outs = (
        jax.ShapeDtypeStruct((ROWS, WIDTH), jnp.bfloat16),
        jax.ShapeDtypeStruct((1, ROWS), jnp.float32),
        jax.ShapeDtypeStruct((N, WIDTH), jnp.bfloat16),
    )
    product = (router_weight * router_gain[:, None]).reshape(1, COLS)
    found = pl.pallas_call(
        kernel,
        out_shape=outs,
        in_specs=[hbm, vmem],
        out_specs=(vmem, vmem, vmem),
        scratch_shapes=[
            pltpu.VMEM((N * ROWS, COLS), jnp.float32),
            pltpu.VMEM((N * ROWS, COLS), jnp.bfloat16),
            pltpu.VMEM((HALF, 8, 128), jnp.float32),
            pltpu.VMEM((N, 8, 128), jnp.float32),
            pltpu.VMEM((HALF, 8, 128), jnp.float32),
            pltpu.VMEM((max(RAW, 16), COLS), jnp.float32),
            pltpu.VMEM((1, 1, COLS), jnp.float32),
            pltpu.VMEM((N, 1, COLS), jnp.float32),
            dma((N,)),
            dma((peers,)), dma((peers,)),
            dma((near,)), dma((near,)),
            dma((peers,)), dma((peers,)),
            dma((owners,)), dma((owners,)),
            dma((1,)), dma((1,)),
            dma((near, 2)), dma((near, 2)),
            dma((1,)), dma((1,)),
        ],
        compiler_params=pltpu.CompilerParams(
            collective_id=0, has_side_effects=True, vmem_limit_bytes=48 << 20
        ),
    )(master_down, product)
    final, scale, router = pl.pallas_call(
        put,
        out_shape=outs,
        in_specs=[vmem, vmem, vmem],
        out_specs=(hbm, hbm, hbm),
        scratch_shapes=[dma((3,))],
        compiler_params=pltpu.CompilerParams(vmem_limit_bytes=4 << 20),
    )(*found)
    return final[None], scale, router.T


def solution(mesh):
    return jax.shard_map(
        per_device,
        mesh=mesh,
        in_specs=(P("owner", None, "rows"), P("rows", "owner"), P("rows")),
        out_specs=(P("owner", "rows", None), P("owner", "rows"), P()),
        check_vma=False,
    )
```

```python
import jax
import jax.numpy as jnp
from jax import lax
from jax.experimental import pallas as pl
from jax.experimental.pallas import tpu as pltpu
from jax.sharding import PartitionSpec as P

MESH = pl.DeviceIdType.MESH
N = 16
HALF = 8
ROWS = 400
COLS = 256
WIDTH = 4096
TILES = ROWS // 8

FAR = [(1, dx, dc) for dx in (0, 2, 1, 3) for dc in (0, 1)]
NEAR = [(0, dx, dc) for dx in (2, 1, 3) for dc in (0, 1)] + [(0, 0, 1)]
PEERS = FAR + NEAR
BACK = [NEAR.index((h, (4 - dx) % 4, dc)) for h, dx, dc in NEAR]
PAIRS = [(dx, dc) for dx in (2, 1, 3, 0) for dc in (1, 0)]
QUAD = 4
FIRST = 208


def peer_row(me, step):
    half, dx, dc = step
    x = lax.rem(lax.rem(me // 2, 4) + dx, 4)
    return lax.rem(me // 8 + half, 2) * 8 + x * 2 + lax.rem(lax.rem(me, 2) + dc, 2)


def sums_of(block, at):
    part = jnp.sum(jnp.abs(block), axis=1, keepdims=True).reshape(TILES, 8, 1)
    shape = (TILES, 8, 128)
    place = lax.broadcasted_iota(jnp.int32, shape, 0) + at == lax.broadcasted_iota(jnp.int32, shape, 2)
    return jnp.sum(jnp.where(place, part, 0.0), axis=0)


def scaled(block, inverse, k):
    by = jnp.concatenate(
        [jnp.broadcast_to(inverse[:, c : c + 1], (8, COLS)) for c in (2 * k, 2 * k + 1)], axis=0
    )
    return (block * by).astype(jnp.bfloat16)


def kernel(
    master_hbm, weight_hbm, gain_hbm, final, scale, router,
    master, narrow, landed, sums, parts, totals, weight, gain, row, quad, column,
    in_sem, small_sem, part_s, part_r, total_s, total_r, tile_s, tile_r, land_s, land_r, on_s, on_r, across_s, across_r, quad_s, quad_r, column_s, column_r, pair_s, pair_r, half_s, half_r,
):
    me, owner = lax.axis_index("rows"), lax.axis_index("owner")
    rows_of = [peer_row(me, step) for step in PEERS]
    across = rows_of[0]
    deep, wide = owner // QUAD, lax.rem(owner, QUAD)
    along_wide = [deep * QUAD + lax.rem(wide + k, QUAD) for k in range(1, QUAD)]
    along_deep = [lax.rem(deep + k, QUAD) * QUAD + wide for k in range(1, QUAD)]
    pair_of = lambda device: lax.rem(device, HALF)

    def send(src, dst, send_sem, recv_sem, to_owner, to_row):
        copy = pltpu.make_async_remote_copy(
            src_ref=src, dst_ref=dst, send_sem=send_sem, recv_sem=recv_sem,
            device_id=(to_owner, to_row), device_id_type=MESH,
        )
        copy.start()
        return copy

    def columns_at(device):
        return pl.ds(pl.multiple_of(device * COLS, COLS), COLS)

    def tile_at(device):
        return pl.ds(pl.multiple_of(device * ROWS, 16), ROWS)

    smalls = [
        pltpu.make_async_copy(src, dst, small_sem.at[i])
        for i, (src, dst) in enumerate(((weight_hbm, weight), (gain_hbm, gain)))
    ]
    for small in smalls:
        small.start()
    loads = []
    for j, (dx, dc) in enumerate(PAIRS):
        q = pair_of(peer_row(me, (0, dx, dc)))
        for h in range(2):
            load = pltpu.make_async_copy(
                master_hbm.at[0, tile_at(q + HALF * h), :], master.at[tile_at(q + HALF * h), :], in_sem.at[j, h]
            )
            load.start()
            loads.append(load)

    barrier = pltpu.get_barrier_semaphore()
    for r in rows_of:
        pl.semaphore_signal(barrier, inc=1, device_id=(owner, r), device_id_type=MESH)
    for o in along_wide + along_deep:
        pl.semaphore_signal(barrier, inc=1, device_id=(o, me), device_id_type=MESH)
    for small in smalls:
        small.wait()
    row[...] = weight[...] * gain[...]
    quad[wide] = weight[...] * gain[...]
    pl.semaphore_wait(barrier, len(rows_of) + 2 * (QUAD - 1))

    quad_copies = [
        send(row, quad.at[wide], quad_s.at[i], quad_r.at[i], o, me) for i, o in enumerate(along_wide)
    ]
    part_copies = []
    for j, (dx, dc) in enumerate(PAIRS):
        q = pair_of(peer_row(me, (0, dx, dc)))
        for h in range(2):
            loads[2 * j + h].wait()
        sums[j] = sums_of(master[tile_at(q), :], 0) + sums_of(master[tile_at(q + HALF), :], TILES)
        if (dx, dc) == (0, 0):
            parts[me] = sums[j]
        for h in (1, 0):
            if (h, dx, dc) in PEERS:
                i = PEERS.index((h, dx, dc))
                part_copies.append(send(sums.at[j], parts.at[me], part_s.at[i], part_r.at[i], owner, rows_of[i]))
    for copy in quad_copies:
        copy.wait_recv()
    column[deep] = quad[...]
    column_copies = [
        send(quad, column.at[deep], column_s.at[i], column_r.at[i], o, me) for i, o in enumerate(along_deep)
    ]
    for copy in part_copies:
        copy.wait_recv()
    total = parts[0]
    for d in range(1, N):
        total = total + parts[d]
    totals[pair_of(me)] = total / WIDTH
    total_copies = [
        send(
            totals.at[pair_of(me)], totals.at[pair_of(me)], total_s.at[i], total_r.at[i], owner, rows_of[len(FAR) + i]
        )
        for i in range(len(NEAR))
    ]

    def mean_of(device):
        both = totals[pair_of(device)]
        return jnp.where(device // HALF == 1, pltpu.roll(both, 128 - TILES, 1), both)

    def inverse_of(device):
        return 1.0 / jnp.where(lax.broadcasted_iota(jnp.int32, (8, 128), 1) < TILES, mean_of(device), 1.0)

    def scale_tile(device, first, last):
        inverse = inverse_of(device)
        for k in range(first // 16, last // 16):
            at = pl.ds(pl.multiple_of(device * ROWS + 16 * k, 16), 16)
            narrow[at, :] = scaled(master[at, :], inverse, k)

    def send_across(s, first, last):
        scale_tile(across, first, last)
        rows = pl.ds(pl.multiple_of(across * ROWS + first, 16), last - first)
        return send(
            narrow.at[rows, :], final.at[pl.ds(first, last - first), columns_at(me)], across_s.at[s], across_r.at[s], owner, across
        )

    across_copies = [send_across(0, 0, FIRST)]
    for copy in column_copies:
        copy.wait_recv()
    block = jnp.concatenate([column[o // QUAD, o % QUAD] for o in range(N)], axis=0)
    router[:, columns_at(me)] = block.astype(jnp.bfloat16)
    land_copies = []
    for j, (_, dx, dc) in enumerate(NEAR):
        total_copies[BACK[j]].wait_recv()
        device = peer_row(me, (1, dx, dc))
        scale_tile(device, 0, ROWS)
        land_copies.append(send(narrow.at[tile_at(device), :], landed.at[j], land_s.at[j], land_r.at[j], owner, across))
        if j == 1:
            pair = send(
                router.at[:, columns_at(me)], router.at[:, columns_at(me)], pair_s.at[0], pair_r.at[0], owner, across
            )
    across_copies.append(send_across(1, FIRST, ROWS))
    tile_copies = []
    for j, (_, dx, dc) in enumerate(NEAR):
        device = peer_row(me, (0, dx, dc))
        scale_tile(device, 0, ROWS)
        tile_copies.append(
            send(narrow.at[tile_at(device), :], final.at[:, columns_at(me)], tile_s.at[j], tile_r.at[j], owner, device)
        )

    own = inverse_of(me)
    for k in range(ROWS // 16):
        block = master[pl.ds(pl.multiple_of(me * ROWS + 16 * k, 16), 16), :]
        final[16 * k : 16 * k + 16, columns_at(me)] = scaled(block, own, k)

    shape = (128, 512)
    spread = (lax.broadcasted_iota(jnp.int32, shape, 1) // 8 == lax.broadcasted_iota(jnp.int32, shape, 0)).astype(jnp.float32)
    wide = jnp.dot(mean_of(me), spread, precision=lax.Precision.HIGHEST, preferred_element_type=jnp.float32)
    shape = (8, 512)
    keep = lax.rem(lax.broadcasted_iota(jnp.int32, shape, 1), 8) == lax.broadcasted_iota(jnp.int32, shape, 0)
    scale[...] = jnp.sum(jnp.where(keep, wide, 0.0), axis=0, keepdims=True)[:, :ROWS]

    half_copies, on_copies = [], []
    for j, (_, dx, dc) in enumerate(NEAR):
        if j == 3:
            pair.wait_recv()
            for n in range(len(NEAR)):
                for k, device in enumerate((me, across)):
                    half_copies.append(
                        send(
                            router.at[:, columns_at(device)], router.at[:, columns_at(device)],
                            half_s.at[n, k], half_r.at[n, k], owner, rows_of[len(FAR) + n],
                        )
                    )
        land_copies[j].wait_recv()
        on_copies.append(
            send(
                landed.at[j], final.at[:, columns_at(across)], on_s.at[j], on_r.at[j], owner, rows_of[len(FAR) + j]
            )
        )
    for copy in quad_copies + column_copies + part_copies + total_copies + land_copies + [pair]:
        copy.wait_send()
    for copy in half_copies + tile_copies + on_copies + across_copies:
        copy.wait()


def put(a, b, c, out_a, out_b, out_c, sem):
    copies = [pltpu.make_async_copy(src, dst, sem.at[i]) for i, (src, dst) in enumerate(((a, out_a), (b, out_b), (c, out_c)))]
    for copy in copies:
        copy.start()
    for copy in copies:
        copy.wait()


def per_device(master_down, router_weight, router_gain):
    vmem, hbm = pl.BlockSpec(memory_space=pltpu.VMEM), pl.BlockSpec(memory_space=pl.ANY)
    dma = pltpu.SemaphoreType.DMA
    peers, near = len(PEERS), len(NEAR)
    outs = (
        jax.ShapeDtypeStruct((ROWS, WIDTH), jnp.bfloat16),
        jax.ShapeDtypeStruct((1, ROWS), jnp.float32),
        jax.ShapeDtypeStruct((N, WIDTH), jnp.bfloat16),
    )
    small = [
        pltpu.with_memory_space_constraint(a.reshape(1, COLS), pltpu.HBM) for a in (router_weight, router_gain)
    ]
    found = pl.pallas_call(
        kernel,
        out_shape=outs,
        in_specs=[hbm, hbm, hbm],
        out_specs=(vmem, vmem, vmem),
        scratch_shapes=[
            pltpu.VMEM((N * ROWS, COLS), jnp.float32),
            pltpu.VMEM((N * ROWS, COLS), jnp.bfloat16),
            pltpu.VMEM((len(NEAR), ROWS, COLS), jnp.bfloat16),
            pltpu.VMEM((HALF, 8, 128), jnp.float32),
            pltpu.VMEM((N, 8, 128), jnp.float32),
            pltpu.VMEM((HALF, 8, 128), jnp.float32),
            pltpu.VMEM((1, COLS), jnp.float32),
            pltpu.VMEM((1, COLS), jnp.float32),
            pltpu.VMEM((1, COLS), jnp.float32),
            pltpu.VMEM((QUAD, 1, COLS), jnp.float32),
            pltpu.VMEM((QUAD, QUAD, 1, COLS), jnp.float32),
            dma((HALF, 2)),
            dma((2,)),
            dma((peers,)), dma((peers,)),
            dma((near,)), dma((near,)),
            dma((near,)), dma((near,)),
            dma((near,)), dma((near,)),
            dma((near,)), dma((near,)),
            dma((2,)), dma((2,)),
            dma((QUAD - 1,)), dma((QUAD - 1,)),
            dma((QUAD - 1,)), dma((QUAD - 1,)),
            dma((1,)), dma((1,)),
            dma((near, 2)), dma((near, 2)),
        ],
        compiler_params=pltpu.CompilerParams(
            collective_id=0, has_side_effects=True, vmem_limit_bytes=50331648
        ),
    )(master_down, *small)
    final, scale, router = pl.pallas_call(
        put,
        out_shape=outs,
        in_specs=[vmem, vmem, vmem],
        out_specs=(hbm, hbm, hbm),
        scratch_shapes=[dma((3,))],
        compiler_params=pltpu.CompilerParams(vmem_limit_bytes=4 << 20),
    )(*found)
    return final[None], scale, router.T


def solution(mesh):
    return jax.shard_map(
        per_device,
        mesh=mesh,
        in_specs=(P("owner", None, "rows"), P("rows", "owner"), P("rows")),
        out_specs=(P("owner", "rows", None), P("owner", "rows"), P()),
        check_vma=False,
    )
```

```python
import jax
import jax.numpy as jnp
from jax import lax
from jax.experimental import pallas as pl
from jax.experimental.pallas import tpu as pltpu
from jax.sharding import PartitionSpec as P

MESH = pl.DeviceIdType.MESH
N = 16
HALF = 8
ROWS = 400
COLS = 256
WIDTH = 4096
TILES = ROWS // 8

FAR = [(1, dx, dc) for dx in (0, 2, 1, 3) for dc in (0, 1)]
NEAR = [(0, dx, dc) for dx in (2, 1, 3) for dc in (0, 1)] + [(0, 0, 1)]
PEERS = FAR + NEAR
BACK = [NEAR.index((h, (4 - dx) % 4, dc)) for h, dx, dc in NEAR]
PAIRS = [(dx, dc) for dx in (2, 1, 3, 0) for dc in (1, 0)]
QUAD = 4
RAW = 112
FIRST = 208


def peer_row(me, step):
    half, dx, dc = step
    x = lax.rem(lax.rem(me // 2, 4) + dx, 4)
    return lax.rem(me // 8 + half, 2) * 8 + x * 2 + lax.rem(lax.rem(me, 2) + dc, 2)


def sums_of(block, at):
    part = jnp.sum(jnp.abs(block), axis=1, keepdims=True).reshape(TILES, 8, 1)
    shape = (TILES, 8, 128)
    place = lax.broadcasted_iota(jnp.int32, shape, 0) + at == lax.broadcasted_iota(jnp.int32, shape, 2)
    return jnp.sum(jnp.where(place, part, 0.0), axis=0)


def scaled(block, inverse, k):
    by = jnp.concatenate(
        [jnp.broadcast_to(inverse[:, c : c + 1], (8, COLS)) for c in (2 * k, 2 * k + 1)], axis=0
    )
    return (block * by).astype(jnp.bfloat16)


def kernel(
    master_hbm, weight_hbm, gain_hbm, final, scale, router,
    master, narrow, landed, raw, sums, parts, totals, weight, gain, row, column, blocks,
    in_sem, small_sem, part_s, part_r, total_s, total_r, tile_s, tile_r, land_s, land_r, on_s, on_r, across_s, across_r, raw_s, raw_r, column_s, column_r, block_s, block_r, pair_s, pair_r, half_s, half_r,
):
    me, owner = lax.axis_index("rows"), lax.axis_index("owner")
    rows_of = [peer_row(me, step) for step in PEERS]
    across = rows_of[0]
    upper = me // HALF
    deep, wide = owner // QUAD, lax.rem(owner, QUAD)
    along_wide = [deep * QUAD + lax.rem(wide + k, QUAD) for k in range(1, QUAD)]
    along_deep = [lax.rem(deep + k, QUAD) * QUAD + wide for k in range(1, QUAD)]
    pair_of = lambda device: lax.rem(device, HALF)

    def send(src, dst, send_sem, recv_sem, to_owner, to_row):
        copy = pltpu.make_async_remote_copy(
            src_ref=src, dst_ref=dst, send_sem=send_sem, recv_sem=recv_sem,
            device_id=(to_owner, to_row), device_id_type=MESH,
        )
        copy.start()
        return copy

    def columns_at(device):
        return pl.ds(pl.multiple_of(device * COLS, COLS), COLS)

    def tile_at(device):
        return pl.ds(pl.multiple_of(device * ROWS, 16), ROWS)

    smalls = [
        pltpu.make_async_copy(src, dst, small_sem.at[i])
        for i, (src, dst) in enumerate(((weight_hbm, weight), (gain_hbm, gain)))
    ]
    for small in smalls:
        small.start()
    loads = []
    for j, (dx, dc) in enumerate(PAIRS):
        q = pair_of(peer_row(me, (0, dx, dc)))
        for h in range(2):
            load = pltpu.make_async_copy(
                master_hbm.at[0, tile_at(q + HALF * h), :], master.at[tile_at(q + HALF * h), :], in_sem.at[j, h]
            )
            load.start()
            loads.append(load)

    barrier = pltpu.get_barrier_semaphore()
    for r in rows_of:
        pl.semaphore_signal(barrier, inc=1, device_id=(owner, r), device_id_type=MESH)
    for o in along_wide + along_deep:
        pl.semaphore_signal(barrier, inc=1, device_id=(o, me), device_id_type=MESH)
    for small in smalls:
        small.wait()
    row[...] = weight[...] * gain[...]
    column[upper, deep] = weight[...] * gain[...]
    pl.semaphore_wait(barrier, len(rows_of) + 2 * (QUAD - 1))

    column_copies = [
        send(row, column.at[upper, deep], column_s.at[i], column_r.at[i], o, me) for i, o in enumerate(along_deep)
    ]
    part_copies = []
    for j, (dx, dc) in enumerate(PAIRS):
        q = pair_of(peer_row(me, (0, dx, dc)))
        for h in range(2):
            loads[2 * j + h].wait()
        sums[j] = sums_of(master[tile_at(q), :], 0) + sums_of(master[tile_at(q + HALF), :], TILES)
        if (dx, dc) == (0, 0):
            parts[me] = sums[j]
        for h in (1, 0):
            if (h, dx, dc) in PEERS:
                i = PEERS.index((h, dx, dc))
                part_copies.append(send(sums.at[j], parts.at[me], part_s.at[i], part_r.at[i], owner, rows_of[i]))
    for copy in column_copies:
        copy.wait_recv()
    pair = send(column.at[upper], column.at[upper], pair_s.at[0], pair_r.at[0], owner, across)
    raw_copy = send(
        master.at[pl.ds(pl.multiple_of(across * ROWS, 16), RAW), :], raw, raw_s.at[0], raw_r.at[0], owner, across
    )
    for copy in part_copies:
        copy.wait_recv()
    total = parts[0]
    for d in range(1, N):
        total = total + parts[d]
    totals[pair_of(me)] = total / WIDTH
    total_copies = [
        send(
            totals.at[pair_of(me)], totals.at[pair_of(me)], total_s.at[i], total_r.at[i], owner, rows_of[len(FAR) + i]
        )
        for i in range(len(NEAR))
    ]

    def mean_of(device):
        both = totals[pair_of(device)]
        return jnp.where(device // HALF == 1, pltpu.roll(both, 128 - TILES, 1), both)

    def inverse_of(device):
        return 1.0 / jnp.where(lax.broadcasted_iota(jnp.int32, (8, 128), 1) < TILES, mean_of(device), 1.0)

    def scale_tile(device, first, last):
        inverse = inverse_of(device)
        for k in range(first // 16, last // 16):
            at = pl.ds(pl.multiple_of(device * ROWS + 16 * k, 16), 16)
            narrow[at, :] = scaled(master[at, :], inverse, k)

    def send_across(s, first, last):
        scale_tile(across, first, last)
        rows = pl.ds(pl.multiple_of(across * ROWS + first, 16), last - first)
        return send(
            narrow.at[rows, :], final.at[pl.ds(first, last - first), columns_at(me)], across_s.at[s], across_r.at[s], owner, across
        )

    across_copies = [send_across(0, RAW, FIRST)]
    land_copies = []
    for j, (_, dx, dc) in enumerate(NEAR):
        total_copies[BACK[j]].wait_recv()
        device = peer_row(me, (1, dx, dc))
        scale_tile(device, 0, ROWS)
        land_copies.append(send(narrow.at[tile_at(device), :], landed.at[j], land_s.at[j], land_r.at[j], owner, across))
    across_copies.append(send_across(1, FIRST, ROWS))
    tile_copies = []
    for j, (_, dx, dc) in enumerate(NEAR):
        device = peer_row(me, (0, dx, dc))
        scale_tile(device, 0, ROWS)
        tile_copies.append(
            send(narrow.at[tile_at(device), :], final.at[:, columns_at(me)], tile_s.at[j], tile_r.at[j], owner, device)
        )

    own = inverse_of(me)
    for k in range(ROWS // 16):
        block = master[pl.ds(pl.multiple_of(me * ROWS + 16 * k, 16), 16), :]
        final[16 * k : 16 * k + 16, columns_at(me)] = scaled(block, own, k)

    raw_copy.wait_recv()
    for k in range(RAW // 16):
        final[16 * k : 16 * k + 16, columns_at(across)] = scaled(raw[16 * k : 16 * k + 16, :], own, k)

    pair.wait_recv()
    blocks[wide] = column[...]
    block_copies = [
        send(column, blocks.at[wide], block_s.at[i], block_r.at[i], o, me) for i, o in enumerate(along_wide)
    ]

    shape = (128, 512)
    spread = (lax.broadcasted_iota(jnp.int32, shape, 1) // 8 == lax.broadcasted_iota(jnp.int32, shape, 0)).astype(jnp.float32)
    wide = jnp.dot(mean_of(me), spread, precision=lax.Precision.HIGHEST, preferred_element_type=jnp.float32)
    shape = (8, 512)
    keep = lax.rem(lax.broadcasted_iota(jnp.int32, shape, 1), 8) == lax.broadcasted_iota(jnp.int32, shape, 0)
    scale[...] = jnp.sum(jnp.where(keep, wide, 0.0), axis=0, keepdims=True)[:, :ROWS]

    for copy in block_copies:
        copy.wait_recv()
    half_copies = []
    for h in range(2):
        lines = [blocks[o % QUAD, h, o // QUAD] for o in range(N)]
        at = columns_at(h * HALF + pair_of(me))
        router[:, at] = jnp.concatenate(lines, axis=0).astype(jnp.bfloat16)
        for n in range(len(NEAR)):
            half_copies.append(
                send(router.at[:, at], router.at[:, at], half_s.at[n, h], half_r.at[n, h], owner, rows_of[len(FAR) + n])
            )

    on_copies = []
    for j in range(len(NEAR)):
        land_copies[j].wait_recv()
        on_copies.append(
            send(
                landed.at[j], final.at[:, columns_at(across)], on_s.at[j], on_r.at[j], owner, rows_of[len(FAR) + j]
            )
        )
    for copy in block_copies + column_copies + part_copies + total_copies + land_copies + [pair, raw_copy]:
        copy.wait_send()
    for copy in half_copies + tile_copies + on_copies + across_copies:
        copy.wait()


def put(a, b, c, out_a, out_b, out_c, sem):
    copies = [pltpu.make_async_copy(src, dst, sem.at[i]) for i, (src, dst) in enumerate(((a, out_a), (b, out_b), (c, out_c)))]
    for copy in copies:
        copy.start()
    for copy in copies:
        copy.wait()


def per_device(master_down, router_weight, router_gain):
    vmem, hbm = pl.BlockSpec(memory_space=pltpu.VMEM), pl.BlockSpec(memory_space=pl.ANY)
    dma = pltpu.SemaphoreType.DMA
    peers, near = len(PEERS), len(NEAR)
    outs = (
        jax.ShapeDtypeStruct((ROWS, WIDTH), jnp.bfloat16),
        jax.ShapeDtypeStruct((1, ROWS), jnp.float32),
        jax.ShapeDtypeStruct((N, WIDTH), jnp.bfloat16),
    )
    small = [
        pltpu.with_memory_space_constraint(a.reshape(1, COLS), pltpu.HBM) for a in (router_weight, router_gain)
    ]
    found = pl.pallas_call(
        kernel,
        out_shape=outs,
        in_specs=[hbm, hbm, hbm],
        out_specs=(vmem, vmem, vmem),
        scratch_shapes=[
            pltpu.VMEM((N * ROWS, COLS), jnp.float32),
            pltpu.VMEM((N * ROWS, COLS), jnp.bfloat16),
            pltpu.VMEM((len(NEAR), ROWS, COLS), jnp.bfloat16),
            pltpu.VMEM((RAW, COLS), jnp.float32),
            pltpu.VMEM((HALF, 8, 128), jnp.float32),
            pltpu.VMEM((N, 8, 128), jnp.float32),
            pltpu.VMEM((HALF, 8, 128), jnp.float32),
            pltpu.VMEM((1, COLS), jnp.float32),
            pltpu.VMEM((1, COLS), jnp.float32),
            pltpu.VMEM((1, COLS), jnp.float32),
            pltpu.VMEM((2, QUAD, 1, COLS), jnp.float32),
            pltpu.VMEM((QUAD, 2, QUAD, 1, COLS), jnp.float32),
            dma((HALF, 2)),
            dma((2,)),
            dma((peers,)), dma((peers,)),
            dma((near,)), dma((near,)),
            dma((near,)), dma((near,)),
            dma((near,)), dma((near,)),
            dma((near,)), dma((near,)),
            dma((2,)), dma((2,)),
            dma((1,)), dma((1,)),
            dma((QUAD - 1,)), dma((QUAD - 1,)),
            dma((QUAD - 1,)), dma((QUAD - 1,)),
            dma((1,)), dma((1,)),
            dma((near, 2)), dma((near, 2)),
        ],
        compiler_params=pltpu.CompilerParams(
            collective_id=0, has_side_effects=True, vmem_limit_bytes=50331648
        ),
    )(master_down, *small)
    final, scale, router = pl.pallas_call(
        put,
        out_shape=outs,
        in_specs=[vmem, vmem, vmem],
        out_specs=(hbm, hbm, hbm),
        scratch_shapes=[dma((3,))],
        compiler_params=pltpu.CompilerParams(vmem_limit_bytes=4 << 20),
    )(*found)
    return final[None], scale, router.T


def solution(mesh):
    return jax.shard_map(
        per_device,
        mesh=mesh,
        in_specs=(P("owner", None, "rows"), P("rows", "owner"), P("rows")),
        out_specs=(P("owner", "rows", None), P("owner", "rows"), P()),
        check_vma=False,
    )
```

```python
import jax
import jax.numpy as jnp
from jax import lax
from jax.experimental import pallas as pl
from jax.experimental.pallas import tpu as pltpu
from jax.sharding import PartitionSpec as P

MESH = pl.DeviceIdType.MESH
N = 16
HALF = 8
ROWS = 400
COLS = 256
WIDTH = 4096
TILES = ROWS // 8

FAR = [(1, dx, dc) for dx in (0, 2, 1, 3) for dc in (0, 1)]
NEAR = [(0, dx, dc) for dx in (2, 1, 3) for dc in (0, 1)] + [(0, 0, 1)]
PEERS = FAR + NEAR
BACK = [NEAR.index((h, (4 - dx) % 4, dc)) for h, dx, dc in NEAR]
PAIRS = [(dx, dc) for dx in (2, 1, 3, 0) for dc in (1, 0)]
QUAD = 4
RAW = 112
EARLY = 6
FIRST = 208


def peer_row(me, step):
    half, dx, dc = step
    x = lax.rem(lax.rem(me // 2, 4) + dx, 4)
    return lax.rem(me // 8 + half, 2) * 8 + x * 2 + lax.rem(lax.rem(me, 2) + dc, 2)


def sums_of(block, at):
    part = jnp.sum(jnp.abs(block), axis=1, keepdims=True).reshape(TILES, 8, 1)
    shape = (TILES, 8, 128)
    place = lax.broadcasted_iota(jnp.int32, shape, 0) + at == lax.broadcasted_iota(jnp.int32, shape, 2)
    return jnp.sum(jnp.where(place, part, 0.0), axis=0)


def scaled(block, inverse, k):
    by = jnp.concatenate(
        [jnp.broadcast_to(inverse[:, c : c + 1], (8, COLS)) for c in (2 * k, 2 * k + 1)], axis=0
    )
    return (block * by).astype(jnp.bfloat16)


def kernel(
    master_hbm, weight_hbm, gain_hbm, final, scale, router,
    master, narrow, landed, raw, sums, parts, totals, weight, gain, row, column, blocks,
    in_sem, small_sem, part_s, part_r, total_s, total_r, tile_s, tile_r, land_s, land_r, on_s, on_r, across_s, across_r, raw_s, raw_r, column_s, column_r, block_s, block_r, pair_s, pair_r, half_s, half_r,
):
    me, owner = lax.axis_index("rows"), lax.axis_index("owner")
    rows_of = [peer_row(me, step) for step in PEERS]
    across = rows_of[0]
    upper = me // HALF
    deep, wide = owner // QUAD, lax.rem(owner, QUAD)
    along_wide = [deep * QUAD + lax.rem(wide + k, QUAD) for k in range(1, QUAD)]
    along_deep = [lax.rem(deep + k, QUAD) * QUAD + wide for k in range(1, QUAD)]
    pair_of = lambda device: lax.rem(device, HALF)

    def send(src, dst, send_sem, recv_sem, to_owner, to_row):
        copy = pltpu.make_async_remote_copy(
            src_ref=src, dst_ref=dst, send_sem=send_sem, recv_sem=recv_sem,
            device_id=(to_owner, to_row), device_id_type=MESH,
        )
        copy.start()
        return copy

    def columns_at(device):
        return pl.ds(pl.multiple_of(device * COLS, COLS), COLS)

    def tile_at(device):
        return pl.ds(pl.multiple_of(device * ROWS, 16), ROWS)

    smalls = [
        pltpu.make_async_copy(src, dst, small_sem.at[i])
        for i, (src, dst) in enumerate(((weight_hbm, weight), (gain_hbm, gain)))
    ]
    for small in smalls:
        small.start()
    loads = []
    for j, (dx, dc) in enumerate(PAIRS):
        q = pair_of(peer_row(me, (0, dx, dc)))
        for h in range(2):
            load = pltpu.make_async_copy(
                master_hbm.at[0, tile_at(q + HALF * h), :], master.at[tile_at(q + HALF * h), :], in_sem.at[j, h]
            )
            load.start()
            loads.append(load)

    barrier = pltpu.get_barrier_semaphore()
    for r in rows_of:
        pl.semaphore_signal(barrier, inc=1, device_id=(owner, r), device_id_type=MESH)
    for o in along_wide + along_deep:
        pl.semaphore_signal(barrier, inc=1, device_id=(o, me), device_id_type=MESH)
    for small in smalls:
        small.wait()
    row[...] = weight[...] * gain[...]
    column[upper, deep] = weight[...] * gain[...]
    def add_up(j, dx, dc):
        q = pair_of(peer_row(me, (0, dx, dc)))
        for h in range(2):
            loads[2 * j + h].wait()
        sums[j] = sums_of(master[tile_at(q), :], 0) + sums_of(master[tile_at(q + HALF), :], TILES)

    for j in range(EARLY):
        add_up(j, *PAIRS[j])
    pl.semaphore_wait(barrier, len(rows_of) + 2 * (QUAD - 1))

    column_copies = [
        send(row, column.at[upper, deep], column_s.at[i], column_r.at[i], o, me) for i, o in enumerate(along_deep)
    ]
    part_copies = []
    for j, (dx, dc) in enumerate(PAIRS):
        if j >= EARLY:
            add_up(j, dx, dc)
        if (dx, dc) == (0, 0):
            parts[me] = sums[j]
        for h in (1, 0):
            if (h, dx, dc) in PEERS:
                i = PEERS.index((h, dx, dc))
                part_copies.append(send(sums.at[j], parts.at[me], part_s.at[i], part_r.at[i], owner, rows_of[i]))
    for copy in column_copies:
        copy.wait_recv()
    pair = send(column.at[upper], column.at[upper], pair_s.at[0], pair_r.at[0], owner, across)
    raw_copy = send(
        master.at[pl.ds(pl.multiple_of(across * ROWS, 16), RAW), :], raw, raw_s.at[0], raw_r.at[0], owner, across
    )
    for copy in part_copies:
        copy.wait_recv()
    total = parts[0]
    for d in range(1, N):
        total = total + parts[d]
    totals[pair_of(me)] = total / WIDTH
    total_copies = [
        send(
            totals.at[pair_of(me)], totals.at[pair_of(me)], total_s.at[i], total_r.at[i], owner, rows_of[len(FAR) + i]
        )
        for i in range(len(NEAR))
    ]

    def mean_of(device):
        both = totals[pair_of(device)]
        return jnp.where(device // HALF == 1, pltpu.roll(both, 128 - TILES, 1), both)

    def inverse_of(device):
        return 1.0 / jnp.where(lax.broadcasted_iota(jnp.int32, (8, 128), 1) < TILES, mean_of(device), 1.0)

    def scale_tile(device, first, last):
        inverse = inverse_of(device)
        for k in range(first // 16, last // 16):
            at = pl.ds(pl.multiple_of(device * ROWS + 16 * k, 16), 16)
            narrow[at, :] = scaled(master[at, :], inverse, k)

    def send_across(s, first, last):
        scale_tile(across, first, last)
        rows = pl.ds(pl.multiple_of(across * ROWS + first, 16), last - first)
        return send(
            narrow.at[rows, :], final.at[pl.ds(first, last - first), columns_at(me)], across_s.at[s], across_r.at[s], owner, across
        )

    across_copies = [send_across(0, RAW, FIRST)]
    land_copies = []
    for j, (_, dx, dc) in enumerate(NEAR):
        total_copies[BACK[j]].wait_recv()
        device = peer_row(me, (1, dx, dc))
        scale_tile(device, 0, ROWS)
        land_copies.append(send(narrow.at[tile_at(device), :], landed.at[j], land_s.at[j], land_r.at[j], owner, across))
    across_copies.append(send_across(1, FIRST, ROWS))
    tile_copies = []
    for j, (_, dx, dc) in enumerate(NEAR):
        device = peer_row(me, (0, dx, dc))
        scale_tile(device, 0, ROWS)
        tile_copies.append(
            send(narrow.at[tile_at(device), :], final.at[:, columns_at(me)], tile_s.at[j], tile_r.at[j], owner, device)
        )

    own = inverse_of(me)
    for k in range(ROWS // 16):
        block = master[pl.ds(pl.multiple_of(me * ROWS + 16 * k, 16), 16), :]
        final[16 * k : 16 * k + 16, columns_at(me)] = scaled(block, own, k)

    raw_copy.wait_recv()
    for k in range(RAW // 16):
        final[16 * k : 16 * k + 16, columns_at(across)] = scaled(raw[16 * k : 16 * k + 16, :], own, k)

    pair.wait_recv()
    blocks[wide] = column[...]
    block_copies = [
        send(column, blocks.at[wide], block_s.at[i], block_r.at[i], o, me) for i, o in enumerate(along_wide)
    ]

    shape = (128, 512)
    spread = (lax.broadcasted_iota(jnp.int32, shape, 1) // 8 == lax.broadcasted_iota(jnp.int32, shape, 0)).astype(jnp.float32)
    wide = jnp.dot(mean_of(me), spread, precision=lax.Precision.HIGHEST, preferred_element_type=jnp.float32)
    shape = (8, 512)
    keep = lax.rem(lax.broadcasted_iota(jnp.int32, shape, 1), 8) == lax.broadcasted_iota(jnp.int32, shape, 0)
    scale[...] = jnp.sum(jnp.where(keep, wide, 0.0), axis=0, keepdims=True)[:, :ROWS]

    for copy in block_copies:
        copy.wait_recv()
    half_copies = []
    for h in range(2):
        lines = [blocks[o % QUAD, h, o // QUAD] for o in range(N)]
        at = columns_at(h * HALF + pair_of(me))
        router[:, at] = jnp.concatenate(lines, axis=0).astype(jnp.bfloat16)
        for n in range(len(NEAR)):
            half_copies.append(
                send(router.at[:, at], router.at[:, at], half_s.at[n, h], half_r.at[n, h], owner, rows_of[len(FAR) + n])
            )

    on_copies = []
    for j in range(len(NEAR)):
        land_copies[j].wait_recv()
        on_copies.append(
            send(
                landed.at[j], final.at[:, columns_at(across)], on_s.at[j], on_r.at[j], owner, rows_of[len(FAR) + j]
            )
        )
    for copy in block_copies + column_copies + part_copies + total_copies + land_copies + [pair, raw_copy]:
        copy.wait_send()
    for copy in half_copies + tile_copies + on_copies + across_copies:
        copy.wait()


def put(a, b, c, out_a, out_b, out_c, sem):
    copies = [pltpu.make_async_copy(src, dst, sem.at[i]) for i, (src, dst) in enumerate(((a, out_a), (b, out_b), (c, out_c)))]
    for copy in copies:
        copy.start()
    for copy in copies:
        copy.wait()


def per_device(master_down, router_weight, router_gain):
    vmem, hbm = pl.BlockSpec(memory_space=pltpu.VMEM), pl.BlockSpec(memory_space=pl.ANY)
    dma = pltpu.SemaphoreType.DMA
    peers, near = len(PEERS), len(NEAR)
    outs = (
        jax.ShapeDtypeStruct((ROWS, WIDTH), jnp.bfloat16),
        jax.ShapeDtypeStruct((1, ROWS), jnp.float32),
        jax.ShapeDtypeStruct((N, WIDTH), jnp.bfloat16),
    )
    small = [
        pltpu.with_memory_space_constraint(a.reshape(1, COLS), pltpu.HBM) for a in (router_weight, router_gain)
    ]
    found = pl.pallas_call(
        kernel,
        out_shape=outs,
        in_specs=[hbm, hbm, hbm],
        out_specs=(vmem, vmem, vmem),
        scratch_shapes=[
            pltpu.VMEM((N * ROWS, COLS), jnp.float32),
            pltpu.VMEM((N * ROWS, COLS), jnp.bfloat16),
            pltpu.VMEM((len(NEAR), ROWS, COLS), jnp.bfloat16),
            pltpu.VMEM((RAW, COLS), jnp.float32),
            pltpu.VMEM((HALF, 8, 128), jnp.float32),
            pltpu.VMEM((N, 8, 128), jnp.float32),
            pltpu.VMEM((HALF, 8, 128), jnp.float32),
            pltpu.VMEM((1, COLS), jnp.float32),
            pltpu.VMEM((1, COLS), jnp.float32),
            pltpu.VMEM((1, COLS), jnp.float32),
            pltpu.VMEM((2, QUAD, 1, COLS), jnp.float32),
            pltpu.VMEM((QUAD, 2, QUAD, 1, COLS), jnp.float32),
            dma((HALF, 2)),
            dma((2,)),
            dma((peers,)), dma((peers,)),
            dma((near,)), dma((near,)),
            dma((near,)), dma((near,)),
            dma((near,)), dma((near,)),
            dma((near,)), dma((near,)),
            dma((2,)), dma((2,)),
            dma((1,)), dma((1,)),
            dma((QUAD - 1,)), dma((QUAD - 1,)),
            dma((QUAD - 1,)), dma((QUAD - 1,)),
            dma((1,)), dma((1,)),
            dma((near, 2)), dma((near, 2)),
        ],
        compiler_params=pltpu.CompilerParams(
            collective_id=0, has_side_effects=True, vmem_limit_bytes=50331648
        ),
    )(master_down, *small)
    final, scale, router = pl.pallas_call(
        put,
        out_shape=outs,
        in_specs=[vmem, vmem, vmem],
        out_specs=(hbm, hbm, hbm),
        scratch_shapes=[dma((3,))],
        compiler_params=pltpu.CompilerParams(vmem_limit_bytes=4 << 20),
    )(*found)
    return final[None], scale, router.T


def solution(mesh):
    return jax.shard_map(
        per_device,
        mesh=mesh,
        in_specs=(P("owner", None, "rows"), P("rows", "owner"), P("rows")),
        out_specs=(P("owner", "rows", None), P("owner", "rows"), P()),
        check_vma=False,
    )
```

```python
import jax
import jax.numpy as jnp
from jax import lax
from jax.experimental import pallas as pl
from jax.experimental.pallas import tpu as pltpu
from jax.sharding import PartitionSpec as P

MESH = pl.DeviceIdType.MESH
N = 16
HALF = 8
ROWS = 400
COLS = 256
WIDTH = 4096
TILES = ROWS // 8

FAR = [(1, dx, dc) for dx in (0, 2, 1, 3) for dc in (0, 1)]
NEAR = [(0, dx, dc) for dx in (2, 1, 3) for dc in (0, 1)] + [(0, 0, 1)]
PEERS = FAR + NEAR
BACK = [NEAR.index((h, (4 - dx) % 4, dc)) for h, dx, dc in NEAR]
PAIRS = [(dx, dc) for dx in (2, 1, 3, 0) for dc in (1, 0)]
QUAD = 4
RAW = 112
EARLY = 6
FIRST = 208


def peer_row(me, step):
    half, dx, dc = step
    x = lax.rem(lax.rem(me // 2, 4) + dx, 4)
    return lax.rem(me // 8 + half, 2) * 8 + x * 2 + lax.rem(lax.rem(me, 2) + dc, 2)


def sums_of(block, at):
    part = jnp.sum(jnp.abs(block), axis=1, keepdims=True).reshape(TILES, 8, 1)
    shape = (TILES, 8, 128)
    place = lax.broadcasted_iota(jnp.int32, shape, 0) + at == lax.broadcasted_iota(jnp.int32, shape, 2)
    return jnp.sum(jnp.where(place, part, 0.0), axis=0)


def scaled(block, inverse, k):
    by = jnp.concatenate(
        [jnp.broadcast_to(inverse[:, c : c + 1], (8, COLS)) for c in (2 * k, 2 * k + 1)], axis=0
    )
    return (block * by).astype(jnp.bfloat16)


def kernel(
    master_hbm, weight_hbm, gain_hbm, final, scale, router,
    master, narrow, landed, raw, sums, parts, totals, weight, gain, row, column, blocks,
    in_sem, small_sem, part_s, part_r, total_s, total_r, tile_s, tile_r, land_s, land_r, on_s, on_r, across_s, across_r, raw_s, raw_r, column_s, column_r, block_s, block_r, pair_s, pair_r, half_s, half_r,
):
    me, owner = lax.axis_index("rows"), lax.axis_index("owner")
    rows_of = [peer_row(me, step) for step in PEERS]
    across = rows_of[0]
    upper = me // HALF
    deep, wide = owner // QUAD, lax.rem(owner, QUAD)
    along_wide = [deep * QUAD + lax.rem(wide + k, QUAD) for k in range(1, QUAD)]
    along_deep = [lax.rem(deep + k, QUAD) * QUAD + wide for k in range(1, QUAD)]
    pair_of = lambda device: lax.rem(device, HALF)

    def send(src, dst, send_sem, recv_sem, to_owner, to_row):
        copy = pltpu.make_async_remote_copy(
            src_ref=src, dst_ref=dst, send_sem=send_sem, recv_sem=recv_sem,
            device_id=(to_owner, to_row), device_id_type=MESH,
        )
        copy.start()
        return copy

    def settle(ref, sem):
        pltpu.make_async_copy(ref, ref, sem).wait()

    def columns_at(device):
        return pl.ds(pl.multiple_of(device * COLS, COLS), COLS)

    def tile_at(device):
        return pl.ds(pl.multiple_of(device * ROWS, 16), ROWS)

    smalls = [
        pltpu.make_async_copy(src, dst, small_sem.at[i])
        for i, (src, dst) in enumerate(((weight_hbm, weight), (gain_hbm, gain)))
    ]
    for small in smalls:
        small.start()
    for j, (dx, dc) in enumerate(PAIRS):
        q = pair_of(peer_row(me, (0, dx, dc)))
        for h in range(2):
            load = pltpu.make_async_copy(
                master_hbm.at[0, tile_at(q + HALF * h), :], master.at[tile_at(q + HALF * h), :], in_sem.at[j]
            )
            load.start()

    barrier = pltpu.get_barrier_semaphore()
    for r in rows_of:
        pl.semaphore_signal(barrier, inc=1, device_id=(owner, r), device_id_type=MESH)
    for o in along_wide + along_deep:
        pl.semaphore_signal(barrier, inc=1, device_id=(o, me), device_id_type=MESH)
    for small in smalls:
        small.wait()
    row[...] = weight[...] * gain[...]
    column[upper, deep] = weight[...] * gain[...]
    def add_up(j, dx, dc):
        q = pair_of(peer_row(me, (0, dx, dc)))
        settle(master.at[pl.ds(0, 2 * ROWS), :], in_sem.at[j])
        sums[j] = sums_of(master[tile_at(q), :], 0) + sums_of(master[tile_at(q + HALF), :], TILES)

    for j in range(EARLY):
        add_up(j, *PAIRS[j])
    pl.semaphore_wait(barrier, len(rows_of) + 2 * (QUAD - 1))

    column_copies = [
        send(row, column.at[upper, deep], column_s.at[0], column_r.at[0], o, me) for i, o in enumerate(along_deep)
    ]
    part_copies = []
    for j, (dx, dc) in enumerate(PAIRS):
        if j >= EARLY:
            add_up(j, dx, dc)
        if (dx, dc) == (0, 0):
            parts[me] = sums[j]
        for h in (1, 0):
            if (h, dx, dc) in PEERS:
                i = PEERS.index((h, dx, dc))
                part_copies.append(send(sums.at[j], parts.at[me], part_s.at[0], part_r.at[0], owner, rows_of[i]))
    three = column.at[0, pl.ds(0, QUAD - 1)]
    settle(three, column_r.at[0])
    pair = send(column.at[upper], column.at[upper], pair_s.at[0], pair_r.at[0], owner, across)
    raw_copy = send(
        master.at[pl.ds(pl.multiple_of(across * ROWS, 16), RAW), :], raw, raw_s.at[0], raw_r.at[0], owner, across
    )
    fifteen = parts.at[pl.ds(0, N - 1)]
    settle(fifteen, part_r.at[0])
    total = parts[0]
    for d in range(1, N):
        total = total + parts[d]
    totals[pair_of(me)] = total / WIDTH
    total_copies = [
        send(
            totals.at[pair_of(me)], totals.at[pair_of(me)], total_s.at[0], total_r.at[i], owner, rows_of[len(FAR) + i]
        )
        for i in range(len(NEAR))
    ]

    def mean_of(device):
        both = totals[pair_of(device)]
        return jnp.where(device // HALF == 1, pltpu.roll(both, 128 - TILES, 1), both)

    def inverse_of(device):
        return 1.0 / jnp.where(lax.broadcasted_iota(jnp.int32, (8, 128), 1) < TILES, mean_of(device), 1.0)

    def scale_tile(device, first, last):
        inverse = inverse_of(device)
        for k in range(first // 16, last // 16):
            at = pl.ds(pl.multiple_of(device * ROWS + 16 * k, 16), 16)
            narrow[at, :] = scaled(master[at, :], inverse, k)

    def send_across(s, first, last):
        scale_tile(across, first, last)
        rows = pl.ds(pl.multiple_of(across * ROWS + first, 16), last - first)
        return send(
            narrow.at[rows, :], final.at[pl.ds(first, last - first), columns_at(me)], across_s.at[0], across_r.at[0], owner, across
        )

    across_copies = [send_across(0, RAW, FIRST)]
    land_copies = []
    for j, (_, dx, dc) in enumerate(NEAR):
        total_copies[BACK[j]].wait_recv()
        device = peer_row(me, (1, dx, dc))
        scale_tile(device, 0, ROWS)
        land_copies.append(send(narrow.at[tile_at(device), :], landed.at[j], land_s.at[0], land_r.at[j], owner, across))
    across_copies.append(send_across(1, FIRST, ROWS))
    tile_copies = []
    for j, (_, dx, dc) in enumerate(NEAR):
        device = peer_row(me, (0, dx, dc))
        scale_tile(device, 0, ROWS)
        tile_copies.append(
            send(narrow.at[tile_at(device), :], final.at[:, columns_at(me)], tile_s.at[0], tile_r.at[0], owner, device)
        )

    own = inverse_of(me)
    for k in range(ROWS // 16):
        block = master[pl.ds(pl.multiple_of(me * ROWS + 16 * k, 16), 16), :]
        final[16 * k : 16 * k + 16, columns_at(me)] = scaled(block, own, k)

    raw_copy.wait_recv()
    for k in range(RAW // 16):
        final[16 * k : 16 * k + 16, columns_at(across)] = scaled(raw[16 * k : 16 * k + 16, :], own, k)

    pair.wait_recv()
    blocks[wide] = column[...]
    block_copies = [
        send(column, blocks.at[wide], block_s.at[0], block_r.at[0], o, me) for i, o in enumerate(along_wide)
    ]

    shape = (128, 512)
    spread = (lax.broadcasted_iota(jnp.int32, shape, 1) // 8 == lax.broadcasted_iota(jnp.int32, shape, 0)).astype(jnp.float32)
    wide = jnp.dot(mean_of(me), spread, precision=lax.Precision.HIGHEST, preferred_element_type=jnp.float32)
    shape = (8, 512)
    keep = lax.rem(lax.broadcasted_iota(jnp.int32, shape, 1), 8) == lax.broadcasted_iota(jnp.int32, shape, 0)
    scale[...] = jnp.sum(jnp.where(keep, wide, 0.0), axis=0, keepdims=True)[:, :ROWS]

    others = blocks.at[pl.ds(0, QUAD - 1)]
    settle(others, block_r.at[0])
    half_copies = []
    for h in range(2):
        lines = [blocks[o % QUAD, h, o // QUAD] for o in range(N)]
        at = columns_at(h * HALF + pair_of(me))
        router[:, at] = jnp.concatenate(lines, axis=0).astype(jnp.bfloat16)
        for n in range(len(NEAR)):
            half_copies.append(
                send(router.at[:, at], router.at[:, at], half_s.at[0], half_r.at[0], owner, rows_of[len(FAR) + n])
            )

    on_copies = []
    for j in range(len(NEAR)):
        land_copies[j].wait_recv()
        on_copies.append(
            send(
                landed.at[j], final.at[:, columns_at(across)], on_s.at[0], on_r.at[0], owner, rows_of[len(FAR) + j]
            )
        )
    for copy in (pair, raw_copy):
        copy.wait_send()
    settle(three, column_s.at[0])
    settle(fifteen, part_s.at[0])
    settle(others, block_s.at[0])
    settle(totals.at[pl.ds(0, len(NEAR))], total_s.at[0])
    settle(landed, land_s.at[0])
    across_part = narrow.at[pl.ds(0, ROWS - RAW), :]
    settle(across_part, across_s.at[0])
    router_part = router.at[:, pl.ds(0, 2 * len(NEAR) * COLS)]
    settle(router_part, half_s.at[0])
    settle(router_part, half_r.at[0])
    for sem in (tile_s, tile_r, on_s, on_r):
        settle(landed, sem.at[0])
    settle(across_part, across_r.at[0])


def put(a, b, c, out_a, out_b, out_c, sem):
    copies = [pltpu.make_async_copy(src, dst, sem.at[i]) for i, (src, dst) in enumerate(((a, out_a), (b, out_b), (c, out_c)))]
    for copy in copies:
        copy.start()
    for copy in copies:
        copy.wait()


def per_device(master_down, router_weight, router_gain):
    vmem, hbm = pl.BlockSpec(memory_space=pltpu.VMEM), pl.BlockSpec(memory_space=pl.ANY)
    dma = pltpu.SemaphoreType.DMA
    near = len(NEAR)
    outs = (
        jax.ShapeDtypeStruct((ROWS, WIDTH), jnp.bfloat16),
        jax.ShapeDtypeStruct((1, ROWS), jnp.float32),
        jax.ShapeDtypeStruct((N, WIDTH), jnp.bfloat16),
    )
    small = [
        pltpu.with_memory_space_constraint(a.reshape(1, COLS), pltpu.HBM) for a in (router_weight, router_gain)
    ]
    found = pl.pallas_call(
        kernel,
        out_shape=outs,
        in_specs=[hbm, hbm, hbm],
        out_specs=(vmem, vmem, vmem),
        scratch_shapes=[
            pltpu.VMEM((N * ROWS, COLS), jnp.float32),
            pltpu.VMEM((N * ROWS, COLS), jnp.bfloat16),
            pltpu.VMEM((len(NEAR), ROWS, COLS), jnp.bfloat16),
            pltpu.VMEM((RAW, COLS), jnp.float32),
            pltpu.VMEM((HALF, 8, 128), jnp.float32),
            pltpu.VMEM((N, 8, 128), jnp.float32),
            pltpu.VMEM((HALF, 8, 128), jnp.float32),
            pltpu.VMEM((1, COLS), jnp.float32),
            pltpu.VMEM((1, COLS), jnp.float32),
            pltpu.VMEM((1, COLS), jnp.float32),
            pltpu.VMEM((2, QUAD, 1, COLS), jnp.float32),
            pltpu.VMEM((QUAD, 2, QUAD, 1, COLS), jnp.float32),
            dma((HALF,)),
            dma((2,)),
            dma((1,)), dma((1,)),
            dma((1,)), dma((near,)),
            dma((1,)), dma((1,)),
            dma((1,)), dma((near,)),
            dma((1,)), dma((1,)),
            dma((1,)), dma((1,)),
            dma((1,)), dma((1,)),
            dma((1,)), dma((1,)),
            dma((1,)), dma((1,)),
            dma((1,)), dma((1,)),
            dma((1,)), dma((1,)),
        ],
        compiler_params=pltpu.CompilerParams(
            collective_id=0, has_side_effects=True, vmem_limit_bytes=50331648
        ),
    )(master_down, *small)
    final, scale, router = pl.pallas_call(
        put,
        out_shape=outs,
        in_specs=[vmem, vmem, vmem],
        out_specs=(hbm, hbm, hbm),
        scratch_shapes=[dma((3,))],
        compiler_params=pltpu.CompilerParams(vmem_limit_bytes=4 << 20),
    )(*found)
    return final[None], scale, router.T


def solution(mesh):
    return jax.shard_map(
        per_device,
        mesh=mesh,
        in_specs=(P("owner", None, "rows"), P("rows", "owner"), P("rows")),
        out_specs=(P("owner", "rows", None), P("owner", "rows"), P()),
        check_vma=False,
    )
```

```python
import jax
import jax.numpy as jnp
from jax import lax
from jax.experimental import pallas as pl
from jax.experimental.pallas import tpu as pltpu
from jax.sharding import PartitionSpec as P

MESH = pl.DeviceIdType.MESH
N = 16
HALF = 8
ROWS = 400
COLS = 256
WIDTH = 4096
TILES = ROWS // 8

FAR = [(1, dx, dc) for dx in (0, 2, 1, 3) for dc in (0, 1)]
NEAR = [(0, dx, dc) for dx in (2, 1, 3) for dc in (0, 1)] + [(0, 0, 1)]
PEERS = FAR + NEAR
BACK = [NEAR.index((h, (4 - dx) % 4, dc)) for h, dx, dc in NEAR]
PAIRS = [(dx, dc) for dx in (2, 1, 3, 0) for dc in (1, 0)]
QUAD = 4
RAW = 112
EARLY = 6
FIRST = 208


def peer_row(me, step):
    half, dx, dc = step
    x = lax.rem(lax.rem(me // 2, 4) + dx, 4)
    return lax.rem(me // 8 + half, 2) * 8 + x * 2 + lax.rem(lax.rem(me, 2) + dc, 2)


def sums_of(block, at):
    part = jnp.sum(jnp.abs(block), axis=1, keepdims=True).reshape(TILES, 8, 1)
    shape = (TILES, 8, 128)
    place = lax.broadcasted_iota(jnp.int32, shape, 0) + at == lax.broadcasted_iota(jnp.int32, shape, 2)
    return jnp.sum(jnp.where(place, part, 0.0), axis=0)


def scaled(block, inverse, k):
    by = jnp.concatenate(
        [jnp.broadcast_to(inverse[:, c : c + 1], (8, COLS)) for c in (2 * k, 2 * k + 1)], axis=0
    )
    return (block * by).astype(jnp.bfloat16)


def kernel(
    master_hbm, weight_hbm, gain_hbm, final, scale, router,
    master, narrow, landed, raw, sums, parts, totals, weight, gain, row, column, blocks,
    in_sem, small_sem, part_s, part_r, total_s, total_r, tile_s, tile_r, land_s, land_r, on_s, on_r, across_s, across_r, raw_s, raw_r, column_s, column_r, block_s, block_r, pair_s, pair_r, half_s, half_r,
):
    me, owner = lax.axis_index("rows"), lax.axis_index("owner")
    rows_of = [peer_row(me, step) for step in PEERS]
    across = rows_of[0]
    upper = me // HALF
    deep, wide = owner // QUAD, lax.rem(owner, QUAD)
    along_wide = [deep * QUAD + lax.rem(wide + k, QUAD) for k in range(1, QUAD)]
    along_deep = [lax.rem(deep + k, QUAD) * QUAD + wide for k in range(1, QUAD)]
    pair_of = lambda device: lax.rem(device, HALF)

    def send(src, dst, send_sem, recv_sem, to_owner, to_row):
        copy = pltpu.make_async_remote_copy(
            src_ref=src, dst_ref=dst, send_sem=send_sem, recv_sem=recv_sem,
            device_id=(to_owner, to_row), device_id_type=MESH,
        )
        copy.start()
        return copy

    def settle(ref, sem):
        pltpu.make_async_copy(ref, ref, sem).wait()

    def columns_at(device):
        return pl.ds(pl.multiple_of(device * COLS, COLS), COLS)

    def tile_at(device):
        return pl.ds(pl.multiple_of(device * ROWS, 16), ROWS)

    smalls = [
        pltpu.make_async_copy(src, dst, small_sem.at[i])
        for i, (src, dst) in enumerate(((weight_hbm, weight), (gain_hbm, gain)))
    ]
    for small in smalls:
        small.start()
    for j, (dx, dc) in enumerate(PAIRS):
        q = pair_of(peer_row(me, (0, dx, dc)))
        for h in range(2):
            load = pltpu.make_async_copy(
                master_hbm.at[0, tile_at(q + HALF * h), :], master.at[tile_at(q + HALF * h), :], in_sem.at[j]
            )
            load.start()

    barrier = pltpu.get_barrier_semaphore()
    for r in rows_of:
        pl.semaphore_signal(barrier, inc=1, device_id=(owner, r), device_id_type=MESH)
    for o in along_wide + along_deep:
        pl.semaphore_signal(barrier, inc=1, device_id=(o, me), device_id_type=MESH)
    for small in smalls:
        small.wait()
    row[...] = weight[...] * gain[...]
    column[upper, deep] = weight[...] * gain[...]
    def add_up(j, dx, dc):
        q = pair_of(peer_row(me, (0, dx, dc)))
        settle(master.at[pl.ds(0, 2 * ROWS), :], in_sem.at[j])
        sums[j] = sums_of(master[tile_at(q), :], 0) + sums_of(master[tile_at(q + HALF), :], TILES)

    for j in range(EARLY):
        add_up(j, *PAIRS[j])
    pl.semaphore_wait(barrier, len(rows_of) + 2 * (QUAD - 1))

    column_copies = [
        send(row, column.at[upper, deep], column_s.at[0], column_r.at[0], o, me) for i, o in enumerate(along_deep)
    ]
    part_copies = []
    for j, (dx, dc) in enumerate(PAIRS):
        if j >= EARLY:
            add_up(j, dx, dc)
        if (dx, dc) == (0, 0):
            parts[me] = sums[j]
        for h in (1, 0):
            if (h, dx, dc) in PEERS:
                i = PEERS.index((h, dx, dc))
                part_copies.append(send(sums.at[j], parts.at[me], part_s.at[0], part_r.at[0], owner, rows_of[i]))
    three = column.at[0, pl.ds(0, QUAD - 1)]
    settle(three, column_r.at[0])
    pair = send(column.at[upper], column.at[upper], pair_s.at[0], pair_r.at[0], owner, across)
    raw_copy = send(
        master.at[pl.ds(pl.multiple_of(across * ROWS, 16), RAW), :], raw, raw_s.at[0], raw_r.at[0], owner, across
    )
    fifteen = parts.at[pl.ds(0, N - 1)]
    settle(fifteen, part_r.at[0])
    total = parts[0]
    for d in range(1, N):
        total = total + parts[d]
    totals[pair_of(me)] = total / WIDTH
    total_copies = [
        send(
            totals.at[pair_of(me)], totals.at[pair_of(me)], total_s.at[0], total_r.at[i], owner, rows_of[len(FAR) + i]
        )
        for i in range(len(NEAR))
    ]

    def mean_of(device):
        both = totals[pair_of(device)]
        return jnp.where(device // HALF == 1, pltpu.roll(both, 128 - TILES, 1), both)

    def inverse_of(device):
        return 1.0 / jnp.where(lax.broadcasted_iota(jnp.int32, (8, 128), 1) < TILES, mean_of(device), 1.0)

    def scale_tile(device, first, last):
        inverse = inverse_of(device)
        for k in range(first // 16, last // 16):
            at = pl.ds(pl.multiple_of(device * ROWS + 16 * k, 16), 16)
            narrow[at, :] = scaled(master[at, :], inverse, k)

    def send_across(s, first, last):
        scale_tile(across, first, last)
        rows = pl.ds(pl.multiple_of(across * ROWS + first, 16), last - first)
        return send(
            narrow.at[rows, :], final.at[pl.ds(first, last - first), columns_at(me)], across_s.at[0], across_r.at[0], owner, across
        )

    across_copies = [send_across(0, RAW, FIRST)]
    land_copies = []
    for j, (_, dx, dc) in enumerate(NEAR):
        total_copies[BACK[j]].wait_recv()
        device = peer_row(me, (1, dx, dc))
        scale_tile(device, 0, ROWS)
        land_copies.append(send(narrow.at[tile_at(device), :], landed.at[j], land_s.at[0], land_r.at[j], owner, across))
    across_copies.append(send_across(1, FIRST, ROWS))
    own = inverse_of(me)
    for k in range(ROWS // 16):
        block = master[pl.ds(pl.multiple_of(me * ROWS + 16 * k, 16), 16), :]
        final[16 * k : 16 * k + 16, columns_at(me)] = scaled(block, own, k)

    raw_copy.wait_recv()
    for k in range(RAW // 16):
        final[16 * k : 16 * k + 16, columns_at(across)] = scaled(raw[16 * k : 16 * k + 16, :], own, k)

    tile_copies = []
    for j, (_, dx, dc) in enumerate(NEAR):
        device = peer_row(me, (0, dx, dc))
        scale_tile(device, 0, ROWS)
        tile_copies.append(
            send(narrow.at[tile_at(device), :], final.at[:, columns_at(me)], tile_s.at[0], tile_r.at[0], owner, device)
        )

    pair.wait_recv()
    blocks[wide] = column[...]
    block_copies = [
        send(column, blocks.at[wide], block_s.at[0], block_r.at[0], o, me) for i, o in enumerate(along_wide)
    ]

    shape = (128, 512)
    spread = (lax.broadcasted_iota(jnp.int32, shape, 1) // 8 == lax.broadcasted_iota(jnp.int32, shape, 0)).astype(jnp.float32)
    wide = jnp.dot(mean_of(me), spread, precision=lax.Precision.HIGHEST, preferred_element_type=jnp.float32)
    shape = (8, 512)
    keep = lax.rem(lax.broadcasted_iota(jnp.int32, shape, 1), 8) == lax.broadcasted_iota(jnp.int32, shape, 0)
    scale[...] = jnp.sum(jnp.where(keep, wide, 0.0), axis=0, keepdims=True)[:, :ROWS]

    others = blocks.at[pl.ds(0, QUAD - 1)]
    settle(others, block_r.at[0])
    half_copies = []
    for h in range(2):
        lines = [blocks[o % QUAD, h, o // QUAD] for o in range(N)]
        at = columns_at(h * HALF + pair_of(me))
        router[:, at] = jnp.concatenate(lines, axis=0).astype(jnp.bfloat16)
        for n in range(len(NEAR)):
            half_copies.append(
                send(router.at[:, at], router.at[:, at], half_s.at[0], half_r.at[0], owner, rows_of[len(FAR) + n])
            )

    on_copies = []
    for j in range(len(NEAR)):
        land_copies[j].wait_recv()
        on_copies.append(
            send(
                landed.at[j], final.at[:, columns_at(across)], on_s.at[0], on_r.at[0], owner, rows_of[len(FAR) + j]
            )
        )
    for copy in (pair, raw_copy):
        copy.wait_send()
    settle(three, column_s.at[0])
    settle(fifteen, part_s.at[0])
    settle(others, block_s.at[0])
    settle(totals.at[pl.ds(0, len(NEAR))], total_s.at[0])
    settle(landed, land_s.at[0])
    across_part = narrow.at[pl.ds(0, ROWS - RAW), :]
    settle(across_part, across_s.at[0])
    router_part = router.at[:, pl.ds(0, 2 * len(NEAR) * COLS)]
    settle(router_part, half_s.at[0])
    settle(router_part, half_r.at[0])
    for sem in (tile_s, tile_r, on_s, on_r):
        settle(landed, sem.at[0])
    settle(across_part, across_r.at[0])


def put(a, b, c, out_a, out_b, out_c, sem):
    copies = [pltpu.make_async_copy(src, dst, sem.at[i]) for i, (src, dst) in enumerate(((a, out_a), (b, out_b), (c, out_c)))]
    for copy in copies:
        copy.start()
    for copy in copies:
        copy.wait()


def per_device(master_down, router_weight, router_gain):
    vmem, hbm = pl.BlockSpec(memory_space=pltpu.VMEM), pl.BlockSpec(memory_space=pl.ANY)
    dma = pltpu.SemaphoreType.DMA
    near = len(NEAR)
    outs = (
        jax.ShapeDtypeStruct((ROWS, WIDTH), jnp.bfloat16),
        jax.ShapeDtypeStruct((1, ROWS), jnp.float32),
        jax.ShapeDtypeStruct((N, WIDTH), jnp.bfloat16),
    )
    small = [
        pltpu.with_memory_space_constraint(a.reshape(1, COLS), pltpu.HBM) for a in (router_weight, router_gain)
    ]
    found = pl.pallas_call(
        kernel,
        out_shape=outs,
        in_specs=[hbm, hbm, hbm],
        out_specs=(vmem, vmem, vmem),
        scratch_shapes=[
            pltpu.VMEM((N * ROWS, COLS), jnp.float32),
            pltpu.VMEM((N * ROWS, COLS), jnp.bfloat16),
            pltpu.VMEM((len(NEAR), ROWS, COLS), jnp.bfloat16),
            pltpu.VMEM((RAW, COLS), jnp.float32),
            pltpu.VMEM((HALF, 8, 128), jnp.float32),
            pltpu.VMEM((N, 8, 128), jnp.float32),
            pltpu.VMEM((HALF, 8, 128), jnp.float32),
            pltpu.VMEM((1, COLS), jnp.float32),
            pltpu.VMEM((1, COLS), jnp.float32),
            pltpu.VMEM((1, COLS), jnp.float32),
            pltpu.VMEM((2, QUAD, 1, COLS), jnp.float32),
            pltpu.VMEM((QUAD, 2, QUAD, 1, COLS), jnp.float32),
            dma((HALF,)),
            dma((2,)),
            dma((1,)), dma((1,)),
            dma((1,)), dma((near,)),
            dma((1,)), dma((1,)),
            dma((1,)), dma((near,)),
            dma((1,)), dma((1,)),
            dma((1,)), dma((1,)),
            dma((1,)), dma((1,)),
            dma((1,)), dma((1,)),
            dma((1,)), dma((1,)),
            dma((1,)), dma((1,)),
            dma((1,)), dma((1,)),
        ],
        compiler_params=pltpu.CompilerParams(
            collective_id=0, has_side_effects=True, vmem_limit_bytes=50331648
        ),
    )(master_down, *small)
    final, scale, router = pl.pallas_call(
        put,
        out_shape=outs,
        in_specs=[vmem, vmem, vmem],
        out_specs=(hbm, hbm, hbm),
        scratch_shapes=[dma((3,))],
        compiler_params=pltpu.CompilerParams(vmem_limit_bytes=4 << 20),
    )(*found)
    return final[None], scale, router.T


def solution(mesh):
    return jax.shard_map(
        per_device,
        mesh=mesh,
        in_specs=(P("owner", None, "rows"), P("rows", "owner"), P("rows")),
        out_specs=(P("owner", "rows", None), P("owner", "rows"), P()),
        check_vma=False,
    )
```

```python
import jax
import jax.numpy as jnp
from jax import lax
from jax.experimental import pallas as pl
from jax.experimental.pallas import tpu as pltpu
from jax.sharding import PartitionSpec as P

MESH = pl.DeviceIdType.MESH
N = 16
HALF = 8
ROWS = 400
COLS = 256
WIDTH = 4096
TILES = ROWS // 8

FAR = [(1, dx, dc) for dx in (0, 2, 1, 3) for dc in (0, 1)]
NEAR = [(0, dx, dc) for dx in (2, 1, 3) for dc in (0, 1)] + [(0, 0, 1)]
PEERS = FAR + NEAR
BACK = [NEAR.index((h, (4 - dx) % 4, dc)) for h, dx, dc in NEAR]
PAIRS = [(dx, dc) for dx in (2, 1, 3, 0) for dc in (1, 0)]
QUAD = 4
RAW = 112
EARLY = 6
FIRST = 208


def peer_row(me, step):
    half, dx, dc = step
    x = lax.rem(lax.rem(me // 2, 4) + dx, 4)
    return lax.rem(me // 8 + half, 2) * 8 + x * 2 + lax.rem(lax.rem(me, 2) + dc, 2)


def sums_of(block, at):
    part = jnp.sum(jnp.abs(block), axis=1, keepdims=True).reshape(TILES, 8, 1)
    shape = (TILES, 8, 128)
    place = lax.broadcasted_iota(jnp.int32, shape, 0) + at == lax.broadcasted_iota(jnp.int32, shape, 2)
    return jnp.sum(jnp.where(place, part, 0.0), axis=0)


def scaled(block, inverse, k):
    by = jnp.concatenate(
        [jnp.broadcast_to(inverse[:, c : c + 1], (8, COLS)) for c in (2 * k, 2 * k + 1)], axis=0
    )
    return (block * by).astype(jnp.bfloat16)


def kernel(
    master_hbm, weight_hbm, gain_hbm, final, scale, router,
    master, narrow, landed, raw, sums, parts, totals, weight, gain, row, column, blocks,
    in_sem, small_sem, part_s, part_r, total_s, total_r, tile_s, tile_r, land_s, land_r, on_s, on_r, across_s, across_r, raw_s, raw_r, column_s, column_r, block_s, block_r, pair_s, pair_r, half_s, half_r,
):
    me, owner = lax.axis_index("rows"), lax.axis_index("owner")
    rows_of = [peer_row(me, step) for step in PEERS]
    across = rows_of[0]
    upper = me // HALF
    deep, wide = owner // QUAD, lax.rem(owner, QUAD)
    along_wide = [deep * QUAD + lax.rem(wide + k, QUAD) for k in range(1, QUAD)]
    along_deep = [lax.rem(deep + k, QUAD) * QUAD + wide for k in range(1, QUAD)]
    pair_of = lambda device: lax.rem(device, HALF)

    def send(src, dst, send_sem, recv_sem, to_owner, to_row):
        copy = pltpu.make_async_remote_copy(
            src_ref=src, dst_ref=dst, send_sem=send_sem, recv_sem=recv_sem,
            device_id=(to_owner, to_row), device_id_type=MESH,
        )
        copy.start()
        return copy

    def settle(ref, sem):
        pltpu.make_async_copy(ref, ref, sem).wait()

    def columns_at(device):
        return pl.ds(pl.multiple_of(device * COLS, COLS), COLS)

    def tile_at(device):
        return pl.ds(pl.multiple_of(device * ROWS, 16), ROWS)

    smalls = [
        pltpu.make_async_copy(src, dst, small_sem.at[i])
        for i, (src, dst) in enumerate(((weight_hbm, weight), (gain_hbm, gain)))
    ]
    for small in smalls:
        small.start()
    for j, (dx, dc) in enumerate(PAIRS):
        q = pair_of(peer_row(me, (0, dx, dc)))
        for h in range(2):
            load = pltpu.make_async_copy(
                master_hbm.at[0, tile_at(q + HALF * h), :], master.at[tile_at(q + HALF * h), :], in_sem.at[j]
            )
            load.start()

    barrier = pltpu.get_barrier_semaphore()
    for r in rows_of:
        pl.semaphore_signal(barrier, inc=1, device_id=(owner, r), device_id_type=MESH)
    for o in along_wide + along_deep:
        pl.semaphore_signal(barrier, inc=1, device_id=(o, me), device_id_type=MESH)
    for small in smalls:
        small.wait()
    row[...] = weight[...] * gain[...]
    column[upper, deep] = weight[...] * gain[...]
    def add_up(j, dx, dc):
        q = pair_of(peer_row(me, (0, dx, dc)))
        settle(master.at[pl.ds(0, 2 * ROWS), :], in_sem.at[j])
        sums[j] = sums_of(master[tile_at(q), :], 0) + sums_of(master[tile_at(q + HALF), :], TILES)

    for j in range(EARLY):
        add_up(j, *PAIRS[j])
    pl.semaphore_wait(barrier, len(rows_of) + 2 * (QUAD - 1))

    column_copies = [
        send(row, column.at[upper, deep], column_s.at[0], column_r.at[0], o, me) for i, o in enumerate(along_deep)
    ]
    part_copies = []
    for j, (dx, dc) in enumerate(PAIRS):
        if j >= EARLY:
            add_up(j, dx, dc)
        if (dx, dc) == (0, 0):
            parts[me] = sums[j]
        for h in (1, 0):
            if (h, dx, dc) in PEERS:
                i = PEERS.index((h, dx, dc))
                part_copies.append(send(sums.at[j], parts.at[me], part_s.at[0], part_r.at[0], owner, rows_of[i]))
    three = column.at[0, pl.ds(0, QUAD - 1)]
    settle(three, column_r.at[0])
    pair = send(column.at[upper], column.at[upper], pair_s.at[0], pair_r.at[0], owner, across)
    raw_copy = send(
        master.at[pl.ds(pl.multiple_of(across * ROWS, 16), RAW), :], raw, raw_s.at[0], raw_r.at[0], owner, across
    )
    fifteen = parts.at[pl.ds(0, N - 1)]
    settle(fifteen, part_r.at[0])
    total = parts[0]
    for d in range(1, N):
        total = total + parts[d]
    totals[pair_of(me)] = total / WIDTH
    total_copies = [
        send(
            totals.at[pair_of(me)], totals.at[pair_of(me)], total_s.at[0], total_r.at[0], owner, rows_of[len(FAR) + i]
        )
        for i in range(len(NEAR))
    ]

    def mean_of(device):
        both = totals[pair_of(device)]
        return jnp.where(device // HALF == 1, pltpu.roll(both, 128 - TILES, 1), both)

    def inverse_of(device):
        return 1.0 / jnp.where(lax.broadcasted_iota(jnp.int32, (8, 128), 1) < TILES, mean_of(device), 1.0)

    def scale_tile(device, first, last):
        inverse = inverse_of(device)
        for k in range(first // 16, last // 16):
            at = pl.ds(pl.multiple_of(device * ROWS + 16 * k, 16), 16)
            narrow[at, :] = scaled(master[at, :], inverse, k)

    def send_across(s, first, last):
        scale_tile(across, first, last)
        rows = pl.ds(pl.multiple_of(across * ROWS + first, 16), last - first)
        return send(
            narrow.at[rows, :], final.at[pl.ds(first, last - first), columns_at(me)], across_s.at[0], across_r.at[0], owner, across
        )

    across_copies = [send_across(0, RAW, FIRST)]
    settle(totals.at[pl.ds(0, len(NEAR))], total_r.at[0])
    land_copies = []
    for j, (_, dx, dc) in enumerate(NEAR):
        device = peer_row(me, (1, dx, dc))
        scale_tile(device, 0, ROWS)
        land_copies.append(send(narrow.at[tile_at(device), :], landed.at[j], land_s.at[0], land_r.at[j], owner, across))
    across_copies.append(send_across(1, FIRST, ROWS))
    tile_copies = []
    for j, (_, dx, dc) in enumerate(NEAR):
        device = peer_row(me, (0, dx, dc))
        scale_tile(device, 0, ROWS)
        tile_copies.append(
            send(narrow.at[tile_at(device), :], final.at[:, columns_at(me)], tile_s.at[0], tile_r.at[0], owner, device)
        )

    own = inverse_of(me)
    for k in range(ROWS // 16):
        block = master[pl.ds(pl.multiple_of(me * ROWS + 16 * k, 16), 16), :]
        final[16 * k : 16 * k + 16, columns_at(me)] = scaled(block, own, k)

    raw_copy.wait_recv()
    for k in range(RAW // 16):
        final[16 * k : 16 * k + 16, columns_at(across)] = scaled(raw[16 * k : 16 * k + 16, :], own, k)

    pair.wait_recv()
    blocks[wide] = column[...]
    block_copies = [
        send(column, blocks.at[wide], block_s.at[0], block_r.at[0], o, me) for i, o in enumerate(along_wide)
    ]

    shape = (128, 512)
    spread = (lax.broadcasted_iota(jnp.int32, shape, 1) // 8 == lax.broadcasted_iota(jnp.int32, shape, 0)).astype(jnp.float32)
    wide = jnp.dot(mean_of(me), spread, precision=lax.Precision.HIGHEST, preferred_element_type=jnp.float32)
    shape = (8, 512)
    keep = lax.rem(lax.broadcasted_iota(jnp.int32, shape, 1), 8) == lax.broadcasted_iota(jnp.int32, shape, 0)
    scale[...] = jnp.sum(jnp.where(keep, wide, 0.0), axis=0, keepdims=True)[:, :ROWS]

    others = blocks.at[pl.ds(0, QUAD - 1)]
    settle(others, block_r.at[0])
    half_copies = []
    for h in range(2):
        lines = [blocks[o % QUAD, h, o // QUAD] for o in range(N)]
        at = columns_at(h * HALF + pair_of(me))
        router[:, at] = jnp.concatenate(lines, axis=0).astype(jnp.bfloat16)
        for n in range(len(NEAR)):
            half_copies.append(
                send(router.at[:, at], router.at[:, at], half_s.at[0], half_r.at[0], owner, rows_of[len(FAR) + n])
            )

    on_copies = []
    for j in range(len(NEAR)):
        land_copies[j].wait_recv()
        on_copies.append(
            send(
                landed.at[j], final.at[:, columns_at(across)], on_s.at[0], on_r.at[0], owner, rows_of[len(FAR) + j]
            )
        )
    for copy in (pair, raw_copy):
        copy.wait_send()
    settle(three, column_s.at[0])
    settle(fifteen, part_s.at[0])
    settle(others, block_s.at[0])
    settle(totals.at[pl.ds(0, len(NEAR))], total_s.at[0])
    settle(landed, land_s.at[0])
    across_part = narrow.at[pl.ds(0, ROWS - RAW), :]
    settle(across_part, across_s.at[0])
    router_part = router.at[:, pl.ds(0, 2 * len(NEAR) * COLS)]
    settle(router_part, half_s.at[0])
    settle(router_part, half_r.at[0])
    for sem in (tile_s, tile_r, on_s, on_r):
        settle(landed, sem.at[0])
    settle(across_part, across_r.at[0])


def put(a, b, c, out_a, out_b, out_c, sem):
    copies = [pltpu.make_async_copy(src, dst, sem.at[i]) for i, (src, dst) in enumerate(((a, out_a), (b, out_b), (c, out_c)))]
    for copy in copies:
        copy.start()
    for copy in copies:
        copy.wait()


def per_device(master_down, router_weight, router_gain):
    vmem, hbm = pl.BlockSpec(memory_space=pltpu.VMEM), pl.BlockSpec(memory_space=pl.ANY)
    dma = pltpu.SemaphoreType.DMA
    near = len(NEAR)
    outs = (
        jax.ShapeDtypeStruct((ROWS, WIDTH), jnp.bfloat16),
        jax.ShapeDtypeStruct((1, ROWS), jnp.float32),
        jax.ShapeDtypeStruct((N, WIDTH), jnp.bfloat16),
    )
    small = [
        pltpu.with_memory_space_constraint(a.reshape(1, COLS), pltpu.HBM) for a in (router_weight, router_gain)
    ]
    found = pl.pallas_call(
        kernel,
        out_shape=outs,
        in_specs=[hbm, hbm, hbm],
        out_specs=(vmem, vmem, vmem),
        scratch_shapes=[
            pltpu.VMEM((N * ROWS, COLS), jnp.float32),
            pltpu.VMEM((N * ROWS, COLS), jnp.bfloat16),
            pltpu.VMEM((len(NEAR), ROWS, COLS), jnp.bfloat16),
            pltpu.VMEM((RAW, COLS), jnp.float32),
            pltpu.VMEM((HALF, 8, 128), jnp.float32),
            pltpu.VMEM((N, 8, 128), jnp.float32),
            pltpu.VMEM((HALF, 8, 128), jnp.float32),
            pltpu.VMEM((1, COLS), jnp.float32),
            pltpu.VMEM((1, COLS), jnp.float32),
            pltpu.VMEM((1, COLS), jnp.float32),
            pltpu.VMEM((2, QUAD, 1, COLS), jnp.float32),
            pltpu.VMEM((QUAD, 2, QUAD, 1, COLS), jnp.float32),
            dma((HALF,)),
            dma((2,)),
            dma((1,)), dma((1,)),
            dma((1,)), dma((1,)),
            dma((1,)), dma((1,)),
            dma((1,)), dma((near,)),
            dma((1,)), dma((1,)),
            dma((1,)), dma((1,)),
            dma((1,)), dma((1,)),
            dma((1,)), dma((1,)),
            dma((1,)), dma((1,)),
            dma((1,)), dma((1,)),
            dma((1,)), dma((1,)),
        ],
        compiler_params=pltpu.CompilerParams(
            collective_id=0, has_side_effects=True, vmem_limit_bytes=50331648
        ),
    )(master_down, *small)
    final, scale, router = pl.pallas_call(
        put,
        out_shape=outs,
        in_specs=[vmem, vmem, vmem],
        out_specs=(hbm, hbm, hbm),
        scratch_shapes=[dma((3,))],
        compiler_params=pltpu.CompilerParams(vmem_limit_bytes=4 << 20),
    )(*found)
    return final[None], scale, router.T


def solution(mesh):
    return jax.shard_map(
        per_device,
        mesh=mesh,
        in_specs=(P("owner", None, "rows"), P("rows", "owner"), P("rows")),
        out_specs=(P("owner", "rows", None), P("owner", "rows"), P()),
        check_vma=False,
    )
```
